128 devices in a mesh: dp: 1, ty: 16 (over z, y), tx: 8 (over x, core).
Axes of the slice: x: 4, y: 4, z: 4, core: 2. Of those that a mesh axis runs over, the one named last changes fastest.
Arguments:
- hidden: bfloat16 [8192, 2048], P(('dp', 'ty'), 'tx')
- positions: int32 [8192], P(('dp', 'tx'))
- g_ffn: bfloat16 [2048], P('tx')
- w_gate: bfloat16 [2048, 8192], P('tx', 'ty')
- w_up: bfloat16 [2048, 8192], P('tx', 'ty')
- w_down: bfloat16 [8192, 2048], P('ty', 'tx')
- g_attn: bfloat16 [2048], P('tx')
- w_q: bfloat16 [2048, 32, 64], P('tx', 'ty')
- w_kv: bfloat16 [2048, 16, 64], P('tx', 'ty')
- grad_h2: bfloat16 [8192, 2048], P(('dp', 'ty'), 'tx')
- grad_q: bfloat16 [8192, 32, 64], P(('dp', 'tx'), 'ty')
- grad_kv: bfloat16 [8192, 16, 64], P(('dp', 'tx'), 'ty')
Outputs:
- output 1: bfloat16 [8192, 2048], P(('dp', 'ty'), 'tx')
- output 2: bfloat16 [8192, 32, 64], P(('dp', 'tx'), 'ty')
- output 3: bfloat16 [8192, 16, 64], P(('dp', 'tx'), 'ty')
- output 4: bfloat16 [8192, 2048], P(('dp', 'ty'), 'tx')
- output 5: float32 [2048], P(('dp', 'tx'))
- output 6: float32 [2048], P(('dp', 'tx'))
- output 7: float32 [2048, 8192], P(('dp', 'tx'), 'ty')
- output 8: float32 [2048, 8192], P(('dp', 'tx'), 'ty')
- output 9: float32 [8192, 2048], P(('dp', 'ty'), 'tx')
- output 10: float32 [2048, 32, 64], P(('dp', 'tx'), 'ty')
- output 11: float32 [2048, 16, 64], P(('dp', 'tx'), 'ty')
All inputs are finite; a program needn't handle non-finite values.
Results may differ from the reference program's by a relative error of at most 0.02.
Values are sent between devices in bfloat16 or wider.
A program may use at most 1 GiB of HBM per device.

```python
import jax
import jax.numpy as jnp
from jax import lax

TOKENS = 8192
MODEL_DIM = 2048
FFN_DIM = 8192
NUM_HEADS = 32
KV_HEADS = 8
HEAD_DIM = 64
MAX_POS = 4096
KV_SLOTS = 2 * KV_HEADS
NORM_EPS = 1e-5
ROPE_BASE = 10000.0


def setup_inputs(seed: int = 0, part: int = 0) -> dict:
    part_keys = jax.random.split(jax.random.fold_in(jax.random.key(seed), part), 7)
    shared_keys = jax.random.split(jax.random.key(seed + 7919), 7)
    row_tilt = jax.random.uniform(part_keys[0], (TOKENS, 1), minval=-0.8, maxval=0.8)
    row_level = jax.random.uniform(part_keys[1], (TOKENS, 1), minval=-0.5, maxval=0.5)
    col_wave = jnp.cos(jnp.pi * (jnp.arange(MODEL_DIM, dtype=jnp.float32) + 0.5) / MODEL_DIM)
    hidden = jax.random.normal(part_keys[2], (TOKENS, MODEL_DIM)) * jnp.exp(row_tilt * col_wave[None, :] + row_level)
    positions = jax.random.randint(part_keys[3], (TOKENS,), 0, MAX_POS, dtype=jnp.int32)
    grad_h2 = jax.random.normal(part_keys[4], (TOKENS, MODEL_DIM))
    grad_q = jax.random.normal(part_keys[5], (TOKENS, NUM_HEADS, HEAD_DIM))
    grad_kv = jax.random.normal(part_keys[6], (TOKENS, KV_SLOTS, HEAD_DIM))
    g_ffn = 1.0 + 0.3 * jax.random.normal(shared_keys[0], (MODEL_DIM,))
    g_attn = 1.0 + 0.3 * jax.random.normal(shared_keys[1], (MODEL_DIM,))
    w_gate = jax.random.normal(shared_keys[2], (MODEL_DIM, FFN_DIM)) * MODEL_DIM ** -0.5
    w_up = jax.random.normal(shared_keys[3], (MODEL_DIM, FFN_DIM)) * MODEL_DIM ** -0.5
    w_down = jax.random.normal(shared_keys[4], (FFN_DIM, MODEL_DIM)) * FFN_DIM ** -0.5
    w_q = jax.random.normal(shared_keys[5], (MODEL_DIM, NUM_HEADS, HEAD_DIM)) * MODEL_DIM ** -0.5
    w_kv = jax.random.normal(shared_keys[6], (MODEL_DIM, KV_SLOTS, HEAD_DIM)) * MODEL_DIM ** -0.5
    return {
        "hidden": hidden.astype(jnp.bfloat16),
        "positions": positions,
        "g_ffn": g_ffn.astype(jnp.bfloat16),
        "w_gate": w_gate.astype(jnp.bfloat16),
        "w_up": w_up.astype(jnp.bfloat16),
        "w_down": w_down.astype(jnp.bfloat16),
        "g_attn": g_attn.astype(jnp.bfloat16),
        "w_q": w_q.astype(jnp.bfloat16),
        "w_kv": w_kv.astype(jnp.bfloat16),
        "grad_h2": grad_h2.astype(jnp.bfloat16),
        "grad_q": grad_q.astype(jnp.bfloat16),
        "grad_kv": grad_kv.astype(jnp.bfloat16),
    }


def rms_scale(values):
    return lax.rsqrt(jnp.mean(values * values, axis=-1, keepdims=True) + NORM_EPS)


def rms_backward(values, inv_rms, gain, grad_out):
    scaled = grad_out * gain.astype(jnp.float32)
    grad_gain = jnp.sum(grad_out * values * inv_rms, axis=0)
    inner_dot = jnp.mean(scaled * values, axis=-1, keepdims=True)
    grad_in = inv_rms * scaled - values * (inv_rms * inv_rms * inv_rms) * inner_dot
    return grad_gain, grad_in


def rope_tables(positions):
    inv_freq = ROPE_BASE ** (-jnp.arange(0, HEAD_DIM, 2, dtype=jnp.float32) / HEAD_DIM)
    angles = positions.astype(jnp.float32)[:, None] * inv_freq[None, :]
    return jnp.cos(angles)[:, None, :], jnp.sin(angles)[:, None, :]


def rotate(values, cos_h, sin_h):
    pair_view = values.reshape(values.shape[:-1] + (values.shape[-1] // 2, 2))
    even_part = pair_view[..., 0]
    odd_part = pair_view[..., 1]
    turned = jnp.stack([even_part * cos_h - odd_part * sin_h, even_part * sin_h + odd_part * cos_h], axis=-1)
    return turned.reshape(values.shape)


def reference(hidden, positions, g_ffn, w_gate, w_up, w_down, g_attn, w_q, w_kv, grad_h2, grad_q, grad_kv):
    hidden_wide = hidden.astype(jnp.float32)
    inv_ffn = rms_scale(hidden_wide)
    normed = (hidden_wide * inv_ffn * g_ffn.astype(jnp.float32)).astype(jnp.bfloat16)
    gate_pre = jnp.dot(normed, w_gate, preferred_element_type=jnp.float32).astype(jnp.bfloat16).astype(jnp.float32)
    up_pre = jnp.dot(normed, w_up, preferred_element_type=jnp.float32).astype(jnp.bfloat16).astype(jnp.float32)
    gate_sig = jax.nn.sigmoid(gate_pre)
    hidden_act = (gate_pre * gate_sig * up_pre).astype(jnp.bfloat16)
    mlp_out = jnp.dot(hidden_act, w_down, preferred_element_type=jnp.float32)
    resid = (hidden_wide + mlp_out).astype(jnp.bfloat16)
    resid_wide = resid.astype(jnp.float32)
    inv_attn = rms_scale(resid_wide)
    normed2 = (resid_wide * inv_attn * g_attn.astype(jnp.float32)).astype(jnp.bfloat16)
    cos_t, sin_t = rope_tables(positions)
    kv_flag = (jnp.arange(KV_SLOTS) < KV_HEADS).astype(jnp.float32)[None, :, None]
    cos_kv = kv_flag * cos_t + (1.0 - kv_flag)
    sin_kv = kv_flag * sin_t
    normed2_wide = normed2.astype(jnp.float32)
    q_proj = jnp.einsum("td,dhk->thk", normed2_wide, w_q.astype(jnp.float32))
    kv_proj = jnp.einsum("td,dhk->thk", normed2_wide, w_kv.astype(jnp.float32))
    q_out = rotate(q_proj, cos_t, sin_t).astype(jnp.bfloat16)
    kv_out = rotate(kv_proj, cos_kv, sin_kv).astype(jnp.bfloat16)
    back_q = rotate(grad_q.astype(jnp.float32), cos_t, -sin_t).astype(jnp.bfloat16).astype(jnp.float32)
    back_kv = rotate(grad_kv.astype(jnp.float32), cos_kv, -sin_kv).astype(jnp.bfloat16).astype(jnp.float32)
    grad_wq = jnp.einsum("td,thk->dhk", normed2_wide, back_q)
    grad_wkv = jnp.einsum("td,thk->dhk", normed2_wide, back_kv)
    grad_n2 = jnp.einsum("thk,dhk->td", back_q, w_q.astype(jnp.float32)) + jnp.einsum("thk,dhk->td", back_kv, w_kv.astype(jnp.float32))
    grad_gattn, grad_attn_in = rms_backward(resid_wide, inv_attn, g_attn, grad_n2)
    grad_res = grad_h2.astype(jnp.float32) + grad_attn_in
    res_half = grad_res.astype(jnp.bfloat16)
    grad_wdown = jnp.dot(hidden_act.T, res_half, preferred_element_type=jnp.float32)
    grad_act = jnp.dot(res_half, w_down.T, preferred_element_type=jnp.float32)
    grad_gate = (grad_act * up_pre * gate_sig * (1.0 + gate_pre * (1.0 - gate_sig))).astype(jnp.bfloat16)
    grad_up = (grad_act * gate_pre * gate_sig).astype(jnp.bfloat16)
    grad_wgate = jnp.dot(normed.T, grad_gate, preferred_element_type=jnp.float32)
    grad_wup = jnp.dot(normed.T, grad_up, preferred_element_type=jnp.float32)
    grad_n = jnp.dot(grad_gate, w_gate.T, preferred_element_type=jnp.float32) + jnp.dot(grad_up, w_up.T, preferred_element_type=jnp.float32)
    grad_gffn, grad_ffn_in = rms_backward(hidden_wide, inv_ffn, g_ffn, grad_n)
    grad_hidden = (grad_res + grad_ffn_in).astype(jnp.bfloat16)
    return (resid, q_out, kv_out, grad_hidden, grad_gffn, grad_gattn, grad_wgate, grad_wup, grad_wdown, grad_wq, grad_wkv)
```

```python
import functools

import jax
import jax.numpy as jnp
from jax import lax
from jax.experimental import pallas as pl
from jax.experimental.pallas import tpu as pltpu
from jax.sharding import PartitionSpec as P

NORM_EPS = 1e-5
ROPE_BASE = 10000.0
RING = 4
CONTRACT_ROWS = (((0,), (0,)), ((), ()))
CONTRACT_COLS = (((1,), (1,)), ((), ()))
BF16 = jnp.bfloat16
F32 = jnp.float32
ORDER = (2, 3, 1, 0)
SPREAD = (0, 3, 1, 2)
BOTH = (0, 1)
SIDES = ((0, 1), (1, -1))
OTHERS = range(1, 8)


def wrap(value, size=RING):
    return lax.rem(value + 2 * size, size)


class Place:
    def __init__(self):
        self.ty = lax.axis_index("ty")
        self.tx = lax.axis_index("tx")
        self.coord = {"z": self.ty // RING, "y": lax.rem(self.ty, RING), "x": self.tx // 2}
        self.core = lax.rem(self.tx, 2)

    def peer(self, axis, delta):
        c = wrap(self.coord[axis] + delta)
        if axis == "x":
            return {"tx": c * 2 + self.core}
        if axis == "z":
            return {"ty": c * RING + self.coord["y"]}
        return {"ty": self.coord["z"] * RING + c}

    def slot(self, axis, delta, other_axis, other_delta):
        c = {axis: wrap(self.coord[axis] + delta), other_axis: wrap(self.coord[other_axis] + other_delta)}
        return c["z"] * RING + c["y"]


def remote(src, dst, sems, index, device):
    send, recv = sems
    return pltpu.make_async_remote_copy(src_ref=src, dst_ref=dst, send_sem=send.at[index], recv_sem=recv.at[index],
                                        device_id=device, device_id_type=pl.DeviceIdType.MESH)


def enter(place, with_ty_all=False):
    barrier = pltpu.get_barrier_semaphore()
    devices = [{"tx": wrap(place.tx + d, 8)} for d in OTHERS]
    if with_ty_all:
        devices += [{"ty": wrap(place.ty + d, 16)} for d in range(1, 16)]
    else:
        devices += [place.peer(axis, d) for axis in ("z", "y") for d in (1, -1)]
    for device in devices:
        pl.semaphore_signal(barrier, inc=1, device_id=device, device_id_type=pl.DeviceIdType.MESH)
    pl.semaphore_wait(barrier, len(devices))


class Exchange:
    def __init__(self, place, piece, out, sems):
        self.place, self.piece, self.out, self.sems = place, piece, out, sems

    def send(self):
        me = self.place.tx
        self.copies = []
        for d in OTHERS:
            to = wrap(me + d, 8)
            copy = remote(self.piece(to), self.out.at[me], self.sems, d - 1, {"tx": to})
            copy.start()
            self.copies.append(copy)

    def own(self):
        self.out[self.place.tx] = self.piece(self.place.tx)[...]

    def recv(self):
        for d in OTHERS:
            src = wrap(self.place.tx - d, 8)
            remote(self.out.at[src], self.out.at[src], self.sems, d - 1, {"tx": src}).wait_recv()

    def done(self):
        for copy in self.copies:
            copy.wait_send()


class TyGather:
    def __init__(self, place, buf, sems):
        self.place, self.buf, self.sems = place, buf, sems
        self.sent = []
        self.quarter = buf.shape[1] // 4

    def message(self, half, phase, d, kind, receiving):
        place = self.place
        first, second = ("z", "y") if half == 0 else ("y", "z")
        axis = first if phase == 0 else second
        side = 1 if kind in (0, 2) else -1
        hops = {0: 0, 1: 0, 2: -1, 3: 1}[kind]
        if receiving:
            hops = hops - side
        if phase == 0:
            slot = place.slot(first, hops, second, 0)
        else:
            slot = place.slot(first, d, second, hops)
        q = self.quarter
        start = 2 * q * half + (q if kind == 3 else 0)
        rows = 2 * q if kind < 2 else q
        ref = self.buf.at[slot, pl.ds(start, rows)]
        index = (half * 5 + (0 if phase == 0 else 1 + d)) * 4 + kind
        return remote(ref, ref, self.sems, index, place.peer(axis, side))

    def send(self, half, phase, d, kinds):
        for kind in kinds:
            copy = self.message(half, phase, d, kind, False)
            copy.start()
            self.sent.append(copy)

    def recv(self, half, phase, d, kind):
        self.message(half, phase, d, kind, True).wait_recv()

    def start(self):
        for half in BOTH:
            self.send(half, 0, 0, BOTH)
        for half in BOTH:
            self.send(half, 1, 0, BOTH)

    def step_first(self):
        for half in BOTH:
            self.recv(half, 0, 0, 0)
            self.send(half, 0, 0, (2,))
            self.recv(half, 0, 0, 1)
            self.send(half, 0, 0, (3,))
        for half in BOTH:
            self.send(half, 1, 3, BOTH)
            self.send(half, 1, 1, BOTH)

    def step_second(self):
        for half in BOTH:
            self.recv(half, 0, 0, 2)
            self.recv(half, 0, 0, 3)
            self.send(half, 1, 2, BOTH)

    def step_forward(self, d):
        for half in BOTH:
            self.recv(half, 1, d, 0)
            self.send(half, 1, d, (2,))
            self.recv(half, 1, d, 1)
            self.send(half, 1, d, (3,))

    def finish(self):
        for d in SPREAD:
            for half in BOTH:
                self.recv(half, 1, d, 2)
                self.recv(half, 1, d, 3)

    def done(self):
        for copy in self.sent:
            copy.wait_send()


GATHER_SEMS = 40


class TyScatter:
    def __init__(self, place, x, got, made, mid, out, sems):
        self.place, self.x, self.got, self.made, self.mid, self.out, self.sems = place, x, got, made, mid, out, sems
        self.sent = []
        self.q = x.shape[1] // 4

    def axes(self, half, phase):
        big, small = ("y", "z") if half == 0 else ("z", "y")
        return (big, small) if phase == 0 else (small, big)

    def part(self, half, phase, d, c, quarter):
        big, small = self.axes(half, 0)
        rows = pl.ds(2 * self.q * half + self.q * quarter, self.q)
        if phase == 0:
            return self.x.at[self.place.slot(big, c, small, d), rows]
        return self.mid.at[half, c % 4, pl.ds(self.q * quarter, self.q)]

    def number(self, half, phase, d):
        return half * 5 + (d if phase == 0 else 4)

    def message(self, half, phase, d, kind):
        n = self.number(half, phase, d)
        side = 1 if kind % 2 == 0 else -1
        axis = self.axes(half, phase)[0]
        if kind == 0:
            src = self.part(half, phase, d, 2, 0)
        elif kind == 1:
            src = self.part(half, phase, d, 2, 1)
        elif kind == 2:
            src = self.part(half, phase, d, 1, 1)
        elif kind == 3:
            src = self.part(half, phase, d, 3, 0)
        else:
            src = self.made.at[n * 2 + kind - 4]
        index = n * 6 + kind
        return remote(src, self.got.at[index], self.sems, index, self.place.peer(axis, side))

    def send(self, half, phase, d, kinds):
        for kind in kinds:
            copy = self.message(half, phase, d, kind)
            copy.start()
            self.sent.append(copy)

    def recv(self, half, phase, d, kind):
        self.message(half, phase, d, kind).wait_recv()
        return self.got[self.number(half, phase, d) * 6 + kind].astype(F32)

    def relay(self, half, phase, d):
        n = self.number(half, phase, d)
        for kind, c, quarter in ((0, 1, 0), (1, 3, 1)):
            got = self.recv(half, phase, d, kind)
            self.made[n * 2 + kind] = (got + self.part(half, phase, d, c, quarter)[...].astype(F32)).astype(BF16)
            self.send(half, phase, d, (4 + kind,))

    def total(self, half, phase, d):
        parts = []
        for quarter in BOTH:
            value = self.part(half, phase, d, 0, quarter)[...].astype(F32)
            value = value + self.recv(half, phase, d, 3 - quarter)
            parts.append(value + self.recv(half, phase, d, 4 + quarter))
        return parts

    def start_relayed(self):
        for d in ORDER:
            for half in BOTH:
                self.send(half, 0, d, BOTH)

    def start_direct(self):
        for d in ORDER:
            for half in BOTH:
                self.send(half, 0, d, (2, 3))

    def relays(self):
        for d in ORDER:
            for half in BOTH:
                self.relay(half, 0, d)

    def middle(self):
        for d in ORDER:
            for half in BOTH:
                parts = self.total(half, 0, d)
                for quarter in BOTH:
                    self.mid[half, d, pl.ds(self.q * quarter, self.q)] = parts[quarter].astype(BF16)
                if d == 2:
                    self.send(half, 1, 0, BOTH)
                elif d == 3:
                    self.send(half, 1, 0, (3,))
                elif d == 1:
                    self.send(half, 1, 0, (2,))

    def last_relay(self):
        for half in BOTH:
            self.relay(half, 1, 0)

    def finish(self):
        for half in BOTH:
            parts = self.total(half, 1, 0)
            for quarter in BOTH:
                self.out[pl.ds(2 * self.q * half + self.q * quarter, self.q)] = parts[quarter]

    def done(self):
        for copy in self.sent:
            copy.wait_send()


SCATTER_SEMS = 60


def scatter_scratch(rows, width):
    q = rows // 4
    return [pltpu.VMEM((SCATTER_SEMS, q, width), BF16), pltpu.VMEM((20, q, width), BF16),
            pltpu.VMEM((2, 4, 2 * q, width), BF16), pltpu.VMEM((rows, width), F32)]


def sem_pair(n):
    return [pltpu.SemaphoreType.DMA((n,)), pltpu.SemaphoreType.DMA((n,))]


class TxGather:
    def __init__(self, place, own, view, sems):
        self.place, self.own_ref, self.view, self.sems = place, own, view, sems
        self.sent = []
        self.rows = own.shape[0]

    def ref(self, delta, part, core=None):
        place = self.place
        core = place.core if core is None else core
        owner = wrap(place.coord["x"] + delta) * 2 + core
        start, rows = {None: (0, self.rows), 0: (0, self.rows // 2), 1: (self.rows // 2, self.rows // 2)}[part]
        return self.view(owner, start, rows)

    def go(self, src, dst, index, device):
        copy = remote(src, dst, self.sems, index, device)
        copy.start()
        self.sent.append(copy)

    def start(self):
        for kind, side in SIDES:
            self.go(self.own_ref, self.ref(0, None), kind, self.place.peer("x", side))
        self.go(self.own_ref, self.ref(0, None), 4, {"tx": self.place.tx + 1 - 2 * self.place.core})

    def own(self):
        self.ref(0, None)[...] = self.own_ref[...]

    def share(self, index, delta):
        ref = self.ref(delta, None)
        self.go(ref, ref, index, {"tx": self.place.tx + 1 - 2 * self.place.core})

    def forward(self):
        for kind, side in SIDES:
            ref = self.ref(-side, None)
            remote(ref, ref, self.sems, kind, self.place.peer("x", side)).wait_recv()
            part = self.ref(-side, kind)
            self.go(part, part, 2 + kind, self.place.peer("x", side))
            self.share(5 + kind, -side)

    def last(self):
        for kind, side in SIDES:
            part = self.ref(2, kind)
            remote(part, part, self.sems, 2 + kind, self.place.peer("x", side)).wait_recv()
        self.share(7, 2)

    def finish(self):
        for index, delta in ((4, 0), (5, -1), (6, 1), (7, 2)):
            ref = self.ref(delta, None, 1 - self.place.core)
            remote(ref, ref, self.sems, index, {"tx": self.place.tx}).wait_recv()

    def done(self):
        for copy in self.sent:
            copy.wait_send()


def block_view(ref):
    return lambda owner, start, rows: ref.at[owner, pl.ds(start, rows)]


def column_view(ref, width):
    return lambda owner, start, rows: ref.at[pl.ds(start, rows), pl.ds(pl.multiple_of(owner * width, width), width)]


def entry_kernel(h, eqkv, gains, wg, wu, wd, wqkv,
                 n_all, h_t, eqkv_t, g_all, wg_all, wu_all, wd_all, wqkv_all,
                 *sems):
    place = Place()
    sems = [sems[2 * k:2 * k + 2] for k in range(len(sems) // 2)]
    width = h.shape[2]
    ex_h = Exchange(place, lambda i: h.at[i], h_t, sems[0])
    ex_g = Exchange(place, lambda i: gains, g_all, sems[1])
    ex_e = Exchange(place, lambda i: eqkv.at[i], eqkv_t, sems[2])
    gather = TyGather(place, n_all, sems[3])
    weights = [TxGather(place, wg, block_view(wg_all), sems[4]), TxGather(place, wu, block_view(wu_all), sems[5]),
               TxGather(place, wd, column_view(wd_all, wd.shape[1]), sems[6]),
               TxGather(place, wqkv, block_view(wqkv_all), sems[7])]
    enter(place)
    ex_h.send()
    ex_g.send()
    weights[0].start()
    weights[1].start()
    ex_h.own()
    ex_g.own()
    ex_h.recv()
    ex_g.recv()
    squares = 0.0
    for i in range(8):
        x = h_t[i].astype(F32)
        squares = squares + jnp.sum(x * x, axis=1, keepdims=True)
    inv = lax.rsqrt(squares / (8 * width) + NORM_EPS)
    for i in range(8):
        x = h_t[i].astype(F32)
        n_all[place.ty, :, i * width:(i + 1) * width] = (x * inv * g_all[i, 0:1]).astype(BF16)
    gather.start()
    weights[2].start()
    weights[3].start()
    ex_e.send()
    for weight in weights:
        weight.own()
    ex_e.own()
    gather.step_first()
    weights[0].forward()
    gather.step_second()
    weights[1].forward()
    gather.step_forward(0)
    weights[2].forward()
    gather.step_forward(3)
    weights[3].forward()
    gather.step_forward(1)
    weights[0].last()
    gather.step_forward(2)
    weights[1].last()
    weights[2].last()
    weights[3].last()
    gather.finish()
    ex_e.recv()
    for weight in weights:
        weight.finish()
    for item in [ex_h, ex_g, ex_e, gather] + weights:
        item.done()


def middle_kernel(x1, x2, h_t, dh2, g_all,
                  n2_all, e_all, resid, dres_t, dg_part,
                  got1, made1, mid1, out1, got2, made2, mid2, out2, h2_t, dh2_t, *sems):
    place = Place()
    sems = [sems[2 * k:2 * k + 2] for k in range(len(sems) // 2)]
    width = dh2.shape[2]
    model_dim = 8 * width
    ex_d = Exchange(place, lambda i: dh2.at[i], dh2_t, sems[0])
    ex_r = Exchange(place, lambda i: h2_t.at[i], resid, sems[1])
    rs1 = TyScatter(place, x1, got1, made1, mid1, out1, sems[2])
    rs2 = TyScatter(place, x2, got2, made2, mid2, out2, sems[3])
    ag1 = TyGather(place, n2_all, sems[4])
    ag2 = TyGather(place, e_all, sems[5])
    enter(place)
    rs1.start_relayed()
    rs1.start_direct()
    ex_d.send()
    ex_d.own()
    rs1.relays()
    rs2.start_relayed()
    rs1.middle()
    rs2.start_direct()
    rs1.last_relay()
    rs2.relays()
    rs1.finish()
    squares = 0.0
    for i in range(8):
        cols = slice(i * width, (i + 1) * width)
        value = (h_t[i].astype(F32) + out1[:, cols]).astype(BF16)
        h2_t[i] = value
        wide = value.astype(F32)
        squares = squares + jnp.sum(wide * wide, axis=1, keepdims=True)
    inv = lax.rsqrt(squares / model_dim + NORM_EPS)
    for i in range(8):
        cols = slice(i * width, (i + 1) * width)
        n2_all[place.ty, :, cols] = (h2_t[i].astype(F32) * inv * g_all[i, 1:2]).astype(BF16)
    ag1.start()
    ex_r.send()
    ex_r.own()
    rs2.middle()
    ag1.step_first()
    rs2.last_relay()
    ag1.step_second()
    rs2.finish()
    ex_d.recv()
    inner = 0.0
    for i in range(8):
        cols = slice(i * width, (i + 1) * width)
        x = h2_t[i].astype(F32)
        grad = out2[:, cols]
        dg_part[i] = jnp.sum(grad * x * inv, axis=0, keepdims=True)
        inner = inner + jnp.sum(grad * g_all[i, 1:2] * x, axis=1, keepdims=True)
    cubed = inv * inv * inv * (inner / model_dim)
    for i in range(8):
        cols = slice(i * width, (i + 1) * width)
        x = h2_t[i].astype(F32)
        value = dh2_t[i].astype(F32) + (inv * (out2[:, cols] * g_all[i, 1:2]) - x * cubed)
        dres_t[i] = value
        e_all[place.ty, :, cols] = value.astype(BF16)
    ag2.start()
    ag1.step_forward(0)
    ag1.step_forward(3)
    ag1.step_forward(1)
    ag2.step_first()
    ag1.step_forward(2)
    ag2.step_second()
    for d in SPREAD:
        ag2.step_forward(d)
    ag1.finish()
    ag2.finish()
    ex_r.recv()
    for item in (ex_d, ex_r, rs1, rs2, ag1, ag2):
        item.done()


class TxScatter:
    def __init__(self, place, view, paired, summed, got, made, out, sems):
        self.place, self.view, self.paired, self.summed = place, view, paired, summed
        self.got, self.made, self.out, self.sems = got, made, out, sems
        self.sent = []
        self.half = out.shape[0] // 2

    def go(self, src, dst, index, device):
        copy = remote(src, dst, self.sems, index, device)
        copy.start()
        self.sent.append(copy)

    def owner(self, d, core):
        return wrap(self.place.coord["x"] + d) * 2 + core

    def start(self):
        place = self.place
        for d in ORDER:
            self.go(self.view(self.owner(d, 1 - place.core)), self.paired.at[d], 6 + d,
                    {"tx": place.tx + 1 - 2 * place.core})

    def pair(self):
        place = self.place
        for d in ORDER:
            remote(self.paired.at[d], self.paired.at[d], self.sems, 6 + d, {"tx": place.tx}).wait_recv()
            mine = self.view(self.owner(d, place.core))
            step = 64

            def body(k, carry, d=d, mine=mine):
                rows = pl.ds(pl.multiple_of(k * step, step), step)
                self.summed[d, rows] = (mine[rows].astype(F32) + self.paired[d, rows].astype(F32)).astype(BF16)
                return carry

            lax.fori_loop(0, self.out.shape[0] // step, body, 0)
            if d == 2:
                self.ring(BOTH)
            elif d == 3:
                self.ring((3,))
            elif d == 1:
                self.ring((2,))

    def message(self, kind):
        side = 1 if kind % 2 == 0 else -1
        if kind < 4:
            d, part = ((2, 0), (2, 1), (1, 1), (3, 0))[kind]
            src = self.summed.at[d, pl.ds(part * self.half, self.half)]
        else:
            src = self.made.at[kind - 4]
        return remote(src, self.got.at[kind], self.sems, kind, self.place.peer("x", side))

    def ring(self, kinds):
        for kind in kinds:
            copy = self.message(kind)
            copy.start()
            self.sent.append(copy)

    def relay(self):
        for kind, d, part in ((0, 1, 0), (1, 3, 1)):
            self.message(kind).wait_recv()
            step = 64

            def body(k, carry, kind=kind, d=d, part=part):
                start = pl.multiple_of(k * step, step)
                rows = pl.ds(start, step)
                theirs = self.summed[d, pl.ds(pl.multiple_of(part * self.half + start, step), step)]
                self.made[kind, rows] = (self.got[kind, rows].astype(F32) + theirs.astype(F32)).astype(BF16)
                return carry

            lax.fori_loop(0, self.half // step, body, 0)
            self.ring((4 + kind,))

    def finish(self):
        for part in BOTH:
            self.message(3 - part).wait_recv()
            self.message(4 + part).wait_recv()
            step = 64

            def body(k, carry, part=part):
                start = pl.multiple_of(k * step, step)
                rows = pl.ds(start, step)
                full = pl.ds(pl.multiple_of(part * self.half + start, step), step)
                value = self.summed[0, full].astype(F32) + self.got[3 - part, rows].astype(F32)
                self.out[full] = value + self.got[4 + part, rows].astype(F32)
                return carry

            lax.fori_loop(0, self.half // step, body, 0)

    def done(self):
        for copy in self.sent:
            copy.wait_send()


TX_SEMS = 10


def tx_scratch(rows, width):
    return [pltpu.VMEM((4, rows, width), BF16), pltpu.VMEM((4, rows, width), BF16),
            pltpu.VMEM((6, rows // 2, width), BF16), pltpu.VMEM((2, rows // 2, width), BF16)]


def exit_kernel(x3, pg, pu, pd, pqkv, qkv, h_t, dres_t, g_all, dg_attn,
                dh, dwg, dwu, dwd, dwqkv, qkv_r, dg_out,
                got3, made3, mid3, out3, *rest):
    place = Place()
    scratch = [rest[4 * k:4 * k + 4] for k in range(4)]
    dh_t, dg_part, dg_x, dg_y = rest[16:20]
    sems = rest[20:]
    sems = [sems[2 * k:2 * k + 2] for k in range(len(sems) // 2)]
    width = h_t.shape[2]
    model_dim = 8 * width
    rs3 = TyScatter(place, x3, got3, made3, mid3, out3, sems[0])
    ex_q = Exchange(place, lambda i: qkv.at[i], qkv_r, sems[1])
    ex_h = Exchange(place, lambda i: dh_t.at[i], dh, sems[2])
    ex_g = Exchange(place, lambda i: dg_part.at[i], dg_x, sems[3])

    def columns(ref):
        return lambda owner: ref.at[:, pl.ds(pl.multiple_of(owner * width, width), width)]

    def blocks(ref):
        return lambda owner: ref.at[owner]

    grads = [TxScatter(place, columns(pd), *scratch[0], dwd, sems[4]), TxScatter(place, blocks(pg), *scratch[1], dwg, sems[5]),
             TxScatter(place, blocks(pu), *scratch[2], dwu, sems[6]), TxScatter(place, blocks(pqkv), *scratch[3], dwqkv, sems[7])]
    enter(place, with_ty_all=True)
    for grad in grads:
        grad.start()
    rs3.start_relayed()
    rs3.start_direct()
    ex_q.send()
    ex_q.own()
    grads[0].pair()
    rs3.relays()
    grads[1].pair()
    grads[2].pair()
    grads[3].pair()
    rs3.middle()
    grads[0].relay()
    grads[1].relay()
    rs3.last_relay()
    grads[2].relay()
    grads[3].relay()
    rs3.finish()
    squares = 0.0
    for i in range(8):
        x = h_t[i].astype(F32)
        squares = squares + jnp.sum(x * x, axis=1, keepdims=True)
    inv = lax.rsqrt(squares / model_dim + NORM_EPS)
    inner = 0.0
    for i in range(8):
        cols = slice(i * width, (i + 1) * width)
        x = h_t[i].astype(F32)
        grad = out3[:, cols]
        dg_part[i, 0:1] = jnp.sum(grad * x * inv, axis=0, keepdims=True)
        dg_part[i, 1:2] = dg_attn[i]
        inner = inner + jnp.sum(grad * g_all[i, 0:1] * x, axis=1, keepdims=True)
    ex_g.send()
    ex_g.own()
    cubed = inv * inv * inv * (inner / model_dim)
    for i in range(8):
        cols = slice(i * width, (i + 1) * width)
        x = h_t[i].astype(F32)
        value = dres_t[i] + (inv * (out3[:, cols] * g_all[i, 0:1]) - x * cubed)
        dh_t[i] = value.astype(BF16)
    ex_h.send()
    ex_h.own()
    ex_g.recv()
    mine = dg_x[0]
    for i in range(1, 8):
        mine = mine + dg_x[i]
    dg_y[place.ty] = mine
    copies = []
    for d in range(1, 16):
        to = wrap(place.ty + d, 16)
        copy = remote(dg_y.at[place.ty], dg_y.at[place.ty], sems[8], d - 1, {"ty": to})
        copy.start()
        copies.append(copy)
    for grad in grads:
        grad.finish()
    for d in range(1, 16):
        src = wrap(place.ty - d, 16)
        remote(dg_y.at[src], dg_y.at[src], sems[8], d - 1, {"ty": src}).wait_recv()
    mine = dg_y[0]
    for j in range(1, 16):
        mine = mine + dg_y[j]
    dg_out[...] = mine
    ex_h.recv()
    ex_q.recv()
    for item in [rs3, ex_q, ex_h, ex_g] + grads:
        item.done()
    for copy in copies:
        copy.wait_send()


def call(kernel, number, outs, scratch, args):
    vmem = pl.BlockSpec(memory_space=pltpu.VMEM)
    return pl.pallas_call(
        kernel, out_shape=[jax.ShapeDtypeStruct(shape, dtype) for shape, dtype in outs],
        in_specs=[vmem] * len(args), out_specs=[vmem] * len(outs), scratch_shapes=scratch,
        compiler_params=pltpu.CompilerParams(collective_id=number, has_side_effects=True), name=kernel.__name__)(*args)


def swap_matrix(size):
    row = lax.broadcasted_iota(jnp.int32, (size, size), 0)
    col = lax.broadcasted_iota(jnp.int32, (size, size), 1)
    return (row == col + 1 - 2 * (col % 2)).astype(BF16)


def solution(mesh):
    ty_size = mesh.shape["ty"]
    tx_size = mesh.shape["tx"]

    def local_step(hidden, positions, g_ffn, w_gate, w_up, w_down, g_attn, w_q, w_kv, grad_h2, grad_q, grad_kv):
        rows, width = hidden.shape
        model_dim = width * tx_size
        ffn = w_gate.shape[1]
        heads_q, head_dim = w_q.shape[1:]
        heads_kv = w_kv.shape[1]
        nq, nkv = heads_q * head_dim, heads_kv * head_dim
        proj = nq + nkv
        tokens = positions.shape[0]
        own = rows // tx_size
        near = tokens // rows

        inv_freq = ROPE_BASE ** (-jnp.arange(0, head_dim, 2, dtype=F32) / head_dim)
        lane_freq = jnp.tile(jnp.repeat(inv_freq, 2), heads_q + heads_kv)
        angles = positions.astype(F32)[:, None] * lane_freq[None, :]
        lane = jnp.arange(proj)
        kv_index = lax.axis_index("ty") * heads_kv + (lane - nq) // head_dim
        turned = (lane < nq) | (kv_index < heads_kv * ty_size // 2)
        cos_t = jnp.where(turned[None, :], jnp.cos(angles), 1.0)
        sin_t = jnp.where(turned[None, :], jnp.sin(angles), 0.0) * jnp.where(lane % 2 == 0, -1.0, 1.0)[None, :]
        swap = swap_matrix(proj)

        back = jnp.concatenate([grad_q.reshape(tokens, nq), grad_kv.reshape(tokens, nkv)], axis=1)
        back_swapped = jnp.dot(back, swap, preferred_element_type=F32)
        eqkv = (back.astype(F32) * cos_t - back_swapped * sin_t).astype(BF16)
        eqkv = eqkv.reshape(near, tx_size, own, proj).transpose(1, 0, 2, 3).reshape(tx_size, near * own, proj)
        w_qkv = jnp.concatenate([w_q.reshape(width, nq), w_kv.reshape(width, nkv)], axis=1)
        gains = jnp.stack([g_ffn.astype(F32), g_attn.astype(F32)])

        block = (ty_size, own, model_dim)
        piece = (tx_size, own, width)
        n_all, h_t, eqkv_t, g_all, wg_all, wu_all, wd_all, wqkv_all = call(
            entry_kernel, 0,
            [(block, BF16), (piece, BF16), ((tx_size, near * own, proj), BF16), ((tx_size, 2, width), F32),
             ((tx_size, width, ffn), BF16), ((tx_size, width, ffn), BF16), ((ffn, model_dim), BF16),
             ((tx_size, width, proj), BF16)],
            sem_pair(7) + sem_pair(7) + sem_pair(7) + sem_pair(GATHER_SEMS) + sem_pair(8) * 4,
            [hidden.reshape(piece), eqkv, gains, w_gate, w_up, w_down, w_qkv])
        n_all = n_all.reshape(tokens, model_dim)
        eqkv_t = eqkv_t.reshape(tokens, proj)
        wg_all = wg_all.reshape(model_dim, ffn)
        wu_all = wu_all.reshape(model_dim, ffn)
        wqkv_all = wqkv_all.reshape(model_dim, proj)

        gate_half = jnp.dot(n_all, wg_all, preferred_element_type=F32).astype(BF16)
        up_half = jnp.dot(n_all, wu_all, preferred_element_type=F32).astype(BF16)
        gate_pre = gate_half.astype(F32)
        up_pre = up_half.astype(F32)
        gate_sig = jax.nn.sigmoid(gate_pre)
        act = (gate_pre * gate_sig * up_pre).astype(BF16)
        down = jnp.dot(act, wd_all, preferred_element_type=F32).astype(BF16)
        n2_part = lax.dot_general(eqkv_t, wqkv_all, CONTRACT_COLS, preferred_element_type=F32).astype(BF16)

        n2_all, e_all, resid, dres_t, dg_attn = call(
            middle_kernel, 1,
            [(block, BF16), (block, BF16), (piece, BF16), (piece, F32), ((tx_size, 1, width), F32)],
            scatter_scratch(own, model_dim) * 2 + [pltpu.VMEM(piece, BF16), pltpu.VMEM(piece, BF16)]
            + sem_pair(7) * 2 + sem_pair(SCATTER_SEMS) * 2 + sem_pair(GATHER_SEMS) * 2,
            [down.reshape(block), n2_part.reshape(block), h_t, grad_h2.reshape(piece), g_all])
        n2_all = n2_all.reshape(tokens, model_dim)
        e_all = e_all.reshape(tokens, model_dim)

        grad_act = lax.dot_general(e_all, wd_all, CONTRACT_COLS, preferred_element_type=F32)
        grad_gate = (grad_act * up_pre * gate_sig * (1.0 + gate_pre * (1.0 - gate_sig))).astype(BF16)
        grad_up = (grad_act * gate_pre * gate_sig).astype(BF16)
        n_part = (lax.dot_general(grad_gate, wg_all, CONTRACT_COLS, preferred_element_type=F32)
                  + lax.dot_general(grad_up, wu_all, CONTRACT_COLS, preferred_element_type=F32)).astype(BF16)
        pg = lax.dot_general(n_all, grad_gate, CONTRACT_ROWS, preferred_element_type=F32).astype(BF16)
        pu = lax.dot_general(n_all, grad_up, CONTRACT_ROWS, preferred_element_type=F32).astype(BF16)
        pd = lax.dot_general(act, e_all, CONTRACT_ROWS, preferred_element_type=F32).astype(BF16)
        pqkv = lax.dot_general(n2_all, eqkv_t, CONTRACT_ROWS, preferred_element_type=F32).astype(BF16)
        qkv = jnp.dot(n2_all, wqkv_all, preferred_element_type=F32).astype(BF16)

        dh, dwg, dwu, dwd, dwqkv, qkv_r, dg = call(
            exit_kernel, 2,
            [(piece, BF16), ((width, ffn), F32), ((width, ffn), F32), ((ffn, width), F32), ((width, proj), F32),
             ((tx_size, near * own, proj), BF16), ((2, width), F32)],
            scatter_scratch(own, model_dim) + tx_scratch(ffn, width) + tx_scratch(width, ffn) * 2 + tx_scratch(width, proj)
            + [pltpu.VMEM(piece, BF16), pltpu.VMEM((tx_size, 2, width), F32), pltpu.VMEM((tx_size, 2, width), F32),
               pltpu.VMEM((ty_size, 2, width), F32)]
            + sem_pair(SCATTER_SEMS) + sem_pair(7) * 3 + sem_pair(TX_SEMS) * 4 + sem_pair(15),
            [n_part.reshape(block), pg.reshape(tx_size, width, ffn), pu.reshape(tx_size, width, ffn), pd,
             pqkv.reshape(tx_size, width, proj), qkv.reshape(tx_size, near * own, proj), h_t, dres_t, g_all, dg_attn])

        qkv_r = qkv_r.reshape(tx_size, near, own, proj).transpose(1, 0, 2, 3).reshape(tokens, proj)
        qkv_swapped = jnp.dot(qkv_r, swap, preferred_element_type=F32)
        qkv_out = (qkv_r.astype(F32) * cos_t + qkv_swapped * sin_t).astype(BF16)
        q_out = qkv_out[:, :nq].reshape(tokens, heads_q, head_dim)
        kv_out = qkv_out[:, nq:].reshape(tokens, heads_kv, head_dim)
        return (resid.reshape(rows, width), q_out, kv_out, dh.reshape(rows, width), dg[0], dg[1], dwg, dwu, dwd,
                dwqkv[:, :nq].reshape(width, heads_q, head_dim), dwqkv[:, nq:].reshape(width, heads_kv, head_dim))

    row_spec = P(("dp", "ty"), "tx")
    head_spec = P(("dp", "tx"), "ty", None)
    in_specs = (row_spec, P(("dp", "tx")), P("tx"), P("tx", "ty"), P("tx", "ty"), P("ty", "tx"), P("tx"), P("tx", "ty", None), P("tx", "ty", None), row_spec, head_spec, head_spec)
    out_specs = (row_spec, head_spec, head_spec, row_spec, P(("dp", "tx")), P(("dp", "tx")), P(("dp", "tx"), "ty"), P(("dp", "tx"), "ty"), P(("dp", "ty"), "tx"), head_spec, head_spec)
    return jax.shard_map(local_step, mesh=mesh, in_specs=in_specs, out_specs=out_specs, check_vma=False)
```

```python
import jax
import jax.numpy as jnp
import numpy as np
from jax import lax
from jax.experimental import pallas as pl
from jax.experimental.pallas import tpu as pltpu
from jax.sharding import PartitionSpec as P

NORM_EPS = 1e-5
ROPE_BASE = 10000.0
RING = 4
TY = 16
TX = 8
NN = (((1,), (0,)), ((), ()))
TN = (((0,), (0,)), ((), ()))
NT = (((1,), (1,)), ((), ()))
BF16 = jnp.bfloat16
F32 = jnp.float32
ORDER = (2, 3, 1, 0)
SPREAD = (0, 3, 1, 2)
BOTH = (0, 1)
SIDES = ((0, 1), (1, -1))
MESH = pl.DeviceIdType.MESH


def wrap(value, size=RING):
    return lax.rem(value + 2 * size, size)


def aligned(start, size, unit=16):
    return pl.ds(pl.multiple_of(start, unit), size)


def chunk(index, size):
    return aligned(index * size, size, size)


def dot(a, b, form):
    return lax.dot_general(a, b, form, preferred_element_type=F32)


class Place:
    def __init__(self):
        self.ty = lax.axis_index("ty")
        self.tx = lax.axis_index("tx")
        self.coord = {"z": self.ty // RING, "y": lax.rem(self.ty, RING), "x": self.tx // 2}
        self.core = lax.rem(self.tx, 2)
        self.sibling = {"tx": self.tx + 1 - 2 * self.core}

    def peer(self, axis, delta):
        c = wrap(self.coord[axis] + delta)
        if axis == "x":
            return {"tx": c * 2 + self.core}
        if axis == "z":
            return {"ty": c * RING + self.coord["y"]}
        return {"ty": self.coord["z"] * RING + c}

    def slot(self, axis, delta, other_axis, other_delta):
        c = {axis: wrap(self.coord[axis] + delta), other_axis: wrap(self.coord[other_axis] + other_delta)}
        return c["z"] * RING + c["y"]


class Link:
    def __init__(self, sems):
        self.send_sem, self.recv_sems = sems

    def make(self, src, dst, index, device):
        return pltpu.make_async_remote_copy(src_ref=src, dst_ref=dst, send_sem=self.send_sem, recv_sem=self.recv_sems.at[index],
                                            device_id=device, device_id_type=MESH)

    def go(self, src, dst, index, device):
        self.make(src, dst, index, device).start()

    def wait(self, ref, index, device):
        self.make(ref, ref, index, device).wait_recv()

    def done(self):
        ref = self.sent()
        self.make(ref, ref, 0, self.place.peer("x", 1)).wait_send()


def enter(devices):
    barrier = pltpu.get_barrier_semaphore()
    for device in devices:
        pl.semaphore_signal(barrier, inc=1, device_id=device, device_id_type=MESH)
    pl.semaphore_wait(barrier, len(devices))


def tx_devices(place):
    return [{"tx": wrap(place.tx + d, TX)} for d in range(1, TX)]


class Exchange(Link):
    def __init__(self, place, piece, out, sems):
        super().__init__(sems)
        self.place, self.piece, self.out = place, piece, out

    def target(self, i):
        return self.out.at[i]

    def send(self):
        place = self.place
        for dx in ORDER:
            for flip in BOTH:
                if dx or flip:
                    to = wrap(place.coord["x"] + dx) * 2 + (1 - place.core if flip else place.core)
                    self.go(self.piece(to), self.target(place.tx), 0, {"tx": to})

    def sent(self):
        return self.out.at[pl.ds(0, self.out.shape[0] - 1)]

    def own(self):
        self.target(self.place.tx)[...] = self.piece(self.place.tx)[...]

    def recv(self):
        self.wait(self.sent(), 0, self.place.sibling)


class TyGather(Link):
    def __init__(self, place, buf, sems):
        super().__init__(sems)
        self.place, self.buf = place, buf
        self.rows = buf.shape[0] // TY

    def message(self, half, phase, d, kind, receiving):
        place = self.place
        first, second = ("z", "y") if half == 0 else ("y", "z")
        axis = second if phase else first
        side = 1 - 2 * (kind % 2)
        hops = (0, 0, -1, 1)[kind]
        if receiving:
            hops = hops - side
        slot = place.slot(first, d, second, hops) if phase else place.slot(first, hops, second, 0)
        q = self.rows // 4
        start = slot * self.rows + 2 * q * half + (q if kind == 3 else 0)
        ref = self.buf.at[aligned(start, 2 * q if kind < 2 else q)]
        number = kind + (0 if not phase else 4 + 2 * d if kind < 2 else 10)
        return ref, half * 14 + number, place.peer(axis, side)

    def send(self, half, phase, d, kinds=BOTH):
        for kind in kinds:
            ref, index, device = self.message(half, phase, d, kind, False)
            self.go(ref, ref, index, device)

    def recv(self, half, phase, d, kind):
        self.wait(*self.message(half, phase, d, kind, True))

    def sent(self):
        return self.buf.at[pl.ds(0, (TY - 1) * self.rows)]

    def start(self):
        for phase in BOTH:
            for half in BOTH:
                self.send(half, phase, 0)

    def relay(self, half, phase, d):
        for kind in BOTH:
            self.recv(half, phase, d, kind)
            self.send(half, phase, d, (2 + kind,))

    def opposite(self, half, phase, d):
        for kind in BOTH:
            self.recv(half, phase, d, 2 + kind)

    def step_first(self):
        for half in BOTH:
            self.relay(half, 0, 0)
        for half in BOTH:
            self.send(half, 1, 3)
            self.send(half, 1, 1)

    def step_second(self):
        for half in BOTH:
            self.opposite(half, 0, 0)
            self.send(half, 1, 2)

    def step_forward(self, d):
        for half in BOTH:
            self.relay(half, 1, d)

    def finish(self):
        for half in BOTH:
            for kind in (2, 3):
                _, index, device = self.message(half, 1, 0, kind, True)
                self.wait(self.buf.at[pl.ds(0, self.rows)], index, device)


class TyScatter(Link):
    def __init__(self, place, x, got, made, mid, out, sems):
        super().__init__(sems)
        self.place, self.x, self.got, self.made, self.mid, self.out = place, x, got, made, mid, out
        self.rows = out.shape[0]
        self.q = self.rows // 4

    def axes(self, half, phase):
        return ("z", "y") if half != phase else ("y", "z")

    def part(self, half, phase, d, c, quarter):
        big, small = self.axes(half, 0)
        if phase:
            return self.mid.at[half, c, pl.ds(self.q * quarter, self.q)]
        start = self.place.slot(big, c, small, d) * self.rows + self.q * (2 * half + quarter)
        return self.x.at[aligned(start, self.q)]

    def number(self, half, phase, d):
        return half * 5 + (4 if phase else d)

    def send(self, half, phase, d, kinds=BOTH):
        n = self.number(half, phase, d)
        for kind in kinds:
            if kind < 4:
                c, quarter = ((2, 0), (2, 1), (1, 1), (3, 0))[kind]
                src = self.part(half, phase, d, c, quarter)
            else:
                src = self.made.at[n * 2 + kind - 4]
            self.go(src, self.got.at[n * 6 + kind], self.semaphore(half, phase, d, kind), self.place.peer(self.axes(half, phase)[0], 1 - 2 * (kind % 2)))

    def semaphore(self, half, phase, d, kind):
        if phase:
            return half * 24 + 18 + kind
        return half * 24 + (14 + kind if kind in (2, 3) else 4 * d + kind % 4 + kind // 4 * 2)

    def recv(self, half, phase, d, kind):
        ref = self.got.at[self.number(half, phase, d) * 6 + kind]
        if phase or kind not in (2, 3):
            self.wait(ref, self.semaphore(half, phase, d, kind), self.place.sibling)
        return ref[...].astype(F32)

    def directs(self):
        for half in BOTH:
            for kind in (2, 3):
                self.wait(self.x.at[pl.ds(0, self.rows)], self.semaphore(half, 0, 0, kind), self.place.sibling)

    def relay(self, half, phase, d):
        n = self.number(half, phase, d)
        for kind in BOTH:
            theirs = self.part(half, phase, d, 1 + 2 * kind, kind)[...].astype(F32)
            self.made[n * 2 + kind] = (self.recv(half, phase, d, kind) + theirs).astype(BF16)
            self.send(half, phase, d, (4 + kind,))

    def total(self, half, phase, d, quarter):
        value = self.part(half, phase, d, 0, quarter)[...].astype(F32)
        value = value + self.recv(half, phase, d, 3 - quarter)
        return value + self.recv(half, phase, d, 4 + quarter)

    def sent(self):
        return self.x.at[pl.ds(0, (TY - 1) * self.rows)]

    def start(self, halves=BOTH):
        for kinds in (BOTH, (2, 3)):
            for d in ORDER:
                for half in halves:
                    self.send(half, 0, d, kinds)

    def fill(self, compute):
        def body(t, carry):
            d = wrap(t + 2)
            compute(wrap(self.place.coord["z"] + d))
            self.send(0, 0, d, range(4))
            return carry

        lax.fori_loop(0, RING, body, 0)
        self.start((1,))

    def relays(self, *ds):
        for d in ds:
            for half in BOTH:
                self.relay(half, 0, d)

    def middle(self, *ds):
        if ds[0] == ORDER[0]:
            self.directs()
        for d in ds:
            for half in BOTH:
                for quarter in BOTH:
                    value = self.total(half, 0, d, quarter)
                    self.mid[half, d, pl.ds(self.q * quarter, self.q)] = value.astype(BF16)
                if d:
                    self.send(half, 1, 0, {2: BOTH, 3: (3,), 1: (2,)}[d])

    def last_relay(self):
        for half in BOTH:
            self.relay(half, 1, 0)

    def finish(self):
        for half in BOTH:
            for quarter in BOTH:
                self.out[pl.ds(self.q * (2 * half + quarter), self.q)] = self.total(half, 1, 0, quarter)


SCATTER_SEMS = 60


def scatter_scratch(rows, width):
    q = rows // 4
    return [pltpu.VMEM((SCATTER_SEMS, q, width), BF16), pltpu.VMEM((20, q, width), BF16),
            pltpu.VMEM((2, 4, 2 * q, width), BF16), pltpu.VMEM((rows, width), F32)]


SEMS = dict(h=1, r=1, g=1, s=1, e=1, q=1, d=1, o=1, ty=1, gate=10, up=5, down=10, proj=10, ag1=28, rs1=48, rs2=48, pair=RING,
            local=13, send=22)


class TxGather(Link):
    def __init__(self, place, own, view, sems):
        super().__init__(sems)
        self.place, self.own_ref, (self.view, self.blocks) = place, own, view
        self.rows = own.shape[0]

    def ref(self, delta, part=None):
        owner = wrap(self.place.coord["x"] + delta) * 2 + self.place.core
        half = self.rows // 2
        return self.view(owner, 0, self.rows) if part is None else self.view(owner, part * half, half)

    def sent(self):
        return self.blocks(TX - 1)

    def start(self):
        for kind, side in SIDES:
            self.go(self.own_ref, self.ref(0), kind, self.place.peer("x", side))
        self.go(self.own_ref, self.ref(0), 4, self.place.sibling)

    def share(self, delta):
        self.go(self.ref(delta), self.ref(delta), 4, self.place.sibling)

    def forward(self):
        for kind, side in SIDES:
            self.wait(self.ref(-side), kind, self.place.peer("x", side))
            part = self.ref(-side, kind)
            self.go(part, part, 2 + kind, self.place.peer("x", side))
            self.share(-side)

    def last(self):
        for kind, side in SIDES:
            self.wait(self.ref(2, kind), 2 + kind, self.place.peer("x", side))
        self.share(2)

    def finish(self):
        self.wait(self.blocks(RING), 4, self.place.sibling)


def row_view(ref, block, columns):
    return (lambda owner, start, rows: ref.at[aligned(owner * block + start, rows), columns],
            lambda n: ref.at[pl.ds(0, n * block), columns])


def column_view(ref, width):
    return (lambda owner, start, rows: ref.at[pl.ds(start, rows), chunk(owner, width)],
            lambda n: ref.at[:, pl.ds(0, n * width)])


class Local:
    def __init__(self, sem):
        self.sem = sem
        self.copies = []

    def go(self, src, dst):
        copy = pltpu.make_async_copy(src, dst, self.sem.at[len(self.copies)])
        copy.start()
        self.copies.append(copy)
        return copy


def swap_rows(value):
    size = value.shape[0]
    row = lax.broadcasted_iota(jnp.int32, (size, size), 0)
    col = lax.broadcasted_iota(jnp.int32, (size, size), 1)
    swap = jnp.where(row == col + 1 - 2 * lax.rem(col, 2), 1.0, 0.0).astype(BF16)
    return dot(swap, value, NN)


def rotated(value, cos_t, sin_t):
    return value.astype(F32) * cos_t + swap_rows(value) * sin_t


def join_halves(left, right, swap_left):
    half = left.shape[1] // 2
    lane = lax.broadcasted_iota(jnp.int32, left.shape, 1)
    if swap_left:
        left = pltpu.roll(left, half, 1)
    else:
        right = pltpu.roll(right, half, 1)
    return jnp.where(lane < half, left, right)


def column(i, width):
    return slice(i * width, (i + 1) * width)


class TxScatter(Link):
    def __init__(self, place, piece, give, paired, got, made, out, sems, pair_sems):
        super().__init__(sems)
        self.pair_sems = pair_sems
        self.place, self.piece, self.give, self.paired, self.summed = place, piece, give, paired, give
        self.got, self.made, self.out = got, made, out
        self.half = out.shape[0] // 2

    def owner(self, d, core):
        return wrap(self.place.coord["x"] + d) * 2 + core

    def handover(self, d):
        return pltpu.make_async_remote_copy(
            src_ref=self.give.at[d], dst_ref=self.paired.at[d], send_sem=self.pair_sems.at[d],
            recv_sem=self.recv_sems.at[6 + d], device_id=self.place.sibling, device_id_type=MESH)

    def sent(self):
        return self.got

    def start(self):
        def body(t, carry):
            d = wrap(t + 2)
            self.give[d] = self.piece(self.owner(d, 1 - self.place.core)).astype(BF16)
            self.handover(d).start()
            return carry

        lax.fori_loop(0, RING, body, 0)

    def pair(self):
        def body(t, carry):
            d = wrap(t + 2)
            value = self.piece(self.owner(d, self.place.core))
            self.handover(d).wait()
            self.summed[d] = (value + self.paired[d].astype(F32)).astype(BF16)
            return carry

        lax.fori_loop(0, RING, body, 0)
        self.ring(range(4))

    def ring(self, kinds):
        for kind in kinds:
            if kind < 4:
                d, part = ((2, 0), (2, 1), (1, 1), (3, 0))[kind]
                src = self.summed.at[d, pl.ds(part * self.half, self.half)]
            else:
                src = self.made.at[kind - 4]
            self.go(src, self.got.at[kind], kind, self.place.peer("x", 1 - 2 * (kind % 2)))

    def each(self, step, count, body):
        def run(k, carry):
            body(k * step)
            return carry

        lax.fori_loop(0, count // step, run, 0)

    def relay(self):
        for kind in BOTH:
            self.wait(self.got.at[kind], kind, self.place.peer("x", 1))

            def body(start, kind=kind):
                rows = aligned(start, 32, 32)
                theirs = self.summed[1 + 2 * kind, aligned(kind * self.half + start, 32, 32)]
                self.made[kind, rows] = (self.got[kind, rows].astype(F32) + theirs.astype(F32)).astype(BF16)

            self.each(32, self.half, body)
            self.ring((4 + kind,))

    def finish(self):
        for part in BOTH:
            for kind in (3 - part, 4 + part):
                self.wait(self.got.at[kind], kind, self.place.peer("x", 1))

            def body(start, part=part):
                rows = aligned(start, 32, 32)
                full = aligned(part * self.half + start, 32, 32)
                value = self.summed[0, full].astype(F32) + self.got[3 - part, rows].astype(F32)
                self.out[full] = value + self.got[4 + part, rows].astype(F32)

            self.each(32, self.half, body)


def tx_scratch(rows, width):
    full = pltpu.VMEM((RING, rows, width), BF16)
    return [full, full, pltpu.VMEM((6, rows // 2, width), BF16), pltpu.VMEM((2, rows // 2, width), BF16)]


def main_kernel(dh2, wg, wu, wd, wq, wkv, *rest):
    inputs, outputs, entered, rest = rest[:7], rest[7:15], rest[15:22], rest[22:]
    h, dq, dkv, positions, freq, g_ffn, g_attn = entered
    resid, dh, q_out, kv_out, dgu, dwd, dproj, dg_out = outputs
    (n_all, wgu, wd_all, wqkv_all, ab, u, eq_t, e_all, x1, x2, eq_send, qkv_r, wqkv, h_t, h2_t, dh2_t, dh_t, dres_t,
     g_all, dg_part, dg_x, dg_y, cos_t, sin_t) = rest[:24]
    rest = rest[24:]
    place = Place()
    rs_scratch1, rs_scratch2 = rest[:4], rest[4:8]
    tx_refs = [rest[8 + 4 * k:12 + 4 * k] for k in range(3)]
    recv, recv_names = rest[20:], list(SEMS)
    local = Local(recv[recv_names.index("local")])
    n2_all, x3, qkv_send, gains = x1, x2, eq_send, dg_y.at[0]
    width = h.shape[2]
    model_dim = TX * width
    ffn = wg.shape[1]
    nq = dq.shape[0]
    head = cos_t.shape[0]
    tile = eq_send.shape[2]
    used = []

    def sems(name):
        used.append(name)
        return recv[recv_names.index("send")].at[len(used) - 1], recv[recv_names.index(name)]

    pair_sems = recv[recv_names.index("pair")]
    ex_h = Exchange(place, lambda i: h.at[i], h_t, sems("h"))
    ex_r = Exchange(place, lambda i: h2_t.at[i], resid, sems("r"))
    ex_g = Exchange(place, lambda i: gains, g_all, sems("g"))
    ex_s = Exchange(place, lambda i: dg_part.at[i], dg_x, sems("s"))
    ex_e = Exchange(place, lambda i: eq_send.at[i], eq_send, sems("e"))
    ex_e.target = lambda i: eq_t.at[:, chunk(i, tile)]
    ex_q = Exchange(place, lambda i: qkv_send.at[i], qkv_r, sems("q"))
    ex_d = Exchange(place, lambda i: dh2.at[i], dh2_t, sems("d"))
    ex_o = Exchange(place, lambda i: dh_t.at[i], dh, sems("o"))
    w_gate = TxGather(place, wg, row_view(wgu, width, pl.ds(0, ffn)), sems("gate"))
    w_up = TxGather(place, wu, row_view(wgu, width, pl.ds(ffn, ffn)), sems("up"))
    w_down = TxGather(place, wd, column_view(wd_all, width), sems("down"))
    w_proj = TxGather(place, wqkv, column_view(wqkv_all, width), sems("proj"))
    down_grad = TxScatter(place, lambda i: dot(u[...], e_all[:, chunk(i, width)], TN), *tx_refs[0], dwd, sems("down"), pair_sems)
    gate_grad = TxScatter(place, lambda i: dot(n_all[:, chunk(i, width)], ab[...], TN), *tx_refs[1], dgu, sems("gate"), pair_sems)
    proj_grad = TxScatter(place, lambda i: dot(eq_t[...], n2_all[:, chunk(i, width)], NN), *tx_refs[2], dproj, sems("proj"),
                          pair_sems)
    gain_link = Exchange(place, None, dg_y, sems("ty"))
    gather = TyGather(place, n_all, sems("ag1"))
    ag_e = TyGather(place, e_all, sems("ag1"))
    ag_n = TyGather(place, n2_all, sems("rs1"))
    rs1 = TyScatter(place, x1, *rs_scratch1, sems("rs1"))
    rs2 = TyScatter(place, x2, *rs_scratch2, sems("rs2"))
    rs3 = TyScatter(place, x3, *rs_scratch2, sems("rs2"))
    entries = [local.go(src, dst) for src, dst in zip(inputs, entered)]
    entries += [local.go(wq, wqkv.at[pl.ds(0, nq)]), local.go(wkv, wqkv.at[pl.ds(nq, wkv.shape[0])])]
    enter(tx_devices(place) + [place.peer(axis, d) for axis in ("z", "y") for d in (1, -1)])
    for copy in entries:
        copy.wait()
    gains[0:1] = g_ffn[...].astype(F32).reshape(1, width)
    gains[1:2] = g_attn[...].astype(F32).reshape(1, width)
    ex_g.send()
    ex_h.send()
    own_copies = [local.go(w.own_ref, w.ref(0)) for w in (w_gate, w_up, w_down)]
    own_copies.append(local.go(dh2.at[place.tx], dh2_t.at[place.tx]))
    angles = freq[...] * positions[...].astype(F32)
    odd_row = lax.rem(lax.broadcasted_iota(jnp.int32, angles.shape, 0), 2) == 1
    cos_t[...] = jnp.cos(angles)
    sine = jnp.sin(angles)
    sin_t[...] = jnp.where(odd_row, sine, -sine)
    turned = place.ty < TY // 2
    for base, ref in ((0, dq), (nq, dkv)):
        for k in range(ref.shape[0] // head):
            rows = slice(k * head, (k + 1) * head)
            out_rows = slice(base + k * head, base + (k + 1) * head)
            value = rotated(ref[rows], cos_t[...], -sin_t[...])
            if base:
                value = jnp.where(turned, value, ref[rows].astype(F32))
            for m in range(TX // 2):
                near, far = value[:, column(m, tile)], value[:, column(m + TX // 2, tile)]
                for odd in BOTH:
                    eq_send[2 * m + odd, out_rows] = join_halves(near, far, odd).astype(BF16)
    ex_e.send()
    w_proj.start()
    w_gate.start()
    ex_e.own()
    w_proj.ref(0)[...] = wqkv[...]
    ex_h.own()
    ex_g.own()
    ex_h.recv()
    ex_g.recv()
    ex_g.done()
    mine = aligned(place.ty * gather.rows, gather.rows)

    def inverse_rms(ref):
        squares = 0.0
        for i in range(TX):
            x = ref[i].astype(F32)
            squares = squares + jnp.sum(x * x, axis=1, keepdims=True)
        return lax.rsqrt(squares / model_dim + NORM_EPS)

    inv1 = inverse_rms(h_t)
    for i in range(TX):
        n_all[mine, column(i, width)] = (h_t[i].astype(F32) * inv1 * g_all[i, 0:1]).astype(BF16)
    gather.start()
    gather.step_first()
    w_proj.forward()
    w_up.start()
    ex_e.recv()
    gather.step_second()
    w_gate.forward()
    w_proj.last()
    gather.step_forward(0)
    w_proj.finish()

    def back_projection(k, carry):
        x2[chunk(k, 256)] = dot(eq_t[:, chunk(k, 256)], wqkv_all[...], TN).astype(BF16)
        return carry

    lax.fori_loop(0, 4, back_projection, 0)
    gather.step_forward(3)
    gather.step_forward(1)
    w_up.forward()
    w_down.start()
    gather.step_forward(2)
    rs2.start()
    w_gate.last()
    gather.finish()
    for copy in own_copies:
        copy.wait()
    w_up.last()
    w_gate.finish()
    w_up.finish()

    def gate_up(k, carry):
        rows = chunk(k, 256)
        both = dot(n_all[rows], wgu[...], NN).astype(BF16)
        ab[rows] = both
        gate = both[:, :ffn].astype(F32)
        u[rows] = (gate * jax.nn.sigmoid(gate) * both[:, ffn:].astype(F32)).astype(BF16)
        return carry

    def down(k):
        x1[chunk(k, 256)] = dot(u[chunk(k, 256)], wd_all[...], NN).astype(BF16)

    lax.fori_loop(0, 2, gate_up, 0)
    w_down.forward()
    ex_d.send()
    rs2.relays(*ORDER)
    lax.fori_loop(2, 4, gate_up, 0)
    w_down.last()
    w_down.finish()
    rs1.fill(down)
    rs2.middle(*ORDER)
    rs1.relays(*ORDER)
    rs2.last_relay()
    rs1.middle(2, 3, 1)
    rs2.finish()
    ex_d.recv()
    rs1.middle(0)
    rs1.last_relay()
    rs2.done()
    rs1.finish()
    for i in range(TX):
        h2_t[i] = (h_t[i].astype(F32) + rs1.out[:, column(i, width)]).astype(BF16)
    inv2 = inverse_rms(h2_t)
    inner = 0.0
    for i in range(TX):
        x = h2_t[i].astype(F32)
        grad = rs2.out[:, column(i, width)]
        dg_part[i, 1:2] = jnp.sum(grad * x * inv2, axis=0, keepdims=True)
        inner = inner + jnp.sum(grad * g_all[i, 1:2] * x, axis=1, keepdims=True)
    cubed = inv2 * inv2 * inv2 * (inner / model_dim)
    for i in range(TX):
        grad = rs2.out[:, column(i, width)] * g_all[i, 1:2]
        value = dh2_t[i].astype(F32) + (inv2 * grad - h2_t[i].astype(F32) * cubed)
        dres_t[i] = value
        e_all[mine, column(i, width)] = value.astype(BF16)
    rs1.done()
    ag_e.start()
    for i in range(TX):
        n2_all[mine, column(i, width)] = (h2_t[i].astype(F32) * inv2 * g_all[i, 1:2]).astype(BF16)
    ex_r.send()
    ex_r.own()
    ag_e.step_first()
    ag_e.step_second()
    for d in SPREAD:
        ag_e.step_forward(d)
    ag_n.start()
    ag_e.finish()

    def grad_act(k, carry):
        rows = chunk(k, 256)
        grad = dot(e_all[rows], wd_all[...], NT)
        gate = ab[rows, :ffn].astype(F32)
        up = ab[rows, ffn:].astype(F32)
        sig = jax.nn.sigmoid(gate)
        ab[rows, :ffn] = (grad * up * sig * (1.0 + gate * (1.0 - sig))).astype(BF16)
        ab[rows, ffn:] = (grad * gate * sig).astype(BF16)
        return carry

    def grad_norm(k):
        x3[chunk(k, 256)] = dot(ab[chunk(k, 256)], wgu[...], NT).astype(BF16)

    def project(k, carry):
        value = dot(wqkv_all[...], n2_all[chunk(k, 256)], NT).astype(BF16)
        qkv_send[2 * k] = value[:, :tile]
        qkv_send[2 * k + 1] = value[:, tile:]
        return carry

    ex_r.recv()
    down_grad.start()
    ag_n.step_first()
    down_grad.pair()
    lax.fori_loop(0, 4, grad_act, 0)
    ag_n.step_second()
    gate_grad.start()
    down_grad.relay()
    ag_n.step_forward(0)
    gate_grad.pair()
    ag_n.step_forward(3)
    ag_n.step_forward(1)
    ag_n.step_forward(2)
    rs3.fill(grad_norm)
    down_grad.finish()
    gate_grad.relay()
    ag_n.finish()
    ex_e.done()
    lax.fori_loop(0, 4, project, 0)
    ex_q.send()
    ex_q.own()
    proj_grad.start()
    rs3.relays(*ORDER)
    proj_grad.pair()
    rs3.middle(*ORDER)
    gate_grad.finish()
    rs3.last_relay()
    proj_grad.relay()
    rs3.finish()
    inner = 0.0
    for i in range(TX):
        x = h_t[i].astype(F32)
        grad = rs3.out[:, column(i, width)]
        dg_part[i, 0:1] = jnp.sum(grad * x * inv1, axis=0, keepdims=True)
        inner = inner + jnp.sum(grad * g_all[i, 0:1] * x, axis=1, keepdims=True)
    ex_s.send()
    ex_s.own()
    cubed = inv1 * inv1 * inv1 * (inner / model_dim)
    for i in range(TX):
        grad = rs3.out[:, column(i, width)] * g_all[i, 0:1]
        dh_t[i] = (dres_t[i] + (inv1 * grad - h_t[i].astype(F32) * cubed)).astype(BF16)
    ex_o.send()
    ex_o.own()
    ex_q.recv()
    for m in range(TX):
        even = 2 * (m % RING)
        cols = column(m, tile)
        left, right = qkv_r[even].astype(F32), qkv_r[even + 1].astype(F32)
        value = join_halves(left, right, m >= RING).astype(BF16)
        for k in range(nq // head):
            q_out[column(k, head), cols] = rotated(value[column(k, head)], cos_t[:, cols], sin_t[:, cols]).astype(BF16)
        for k in range(kv_out.shape[0] // head):
            part = value[nq + k * head:nq + (k + 1) * head]
            spun = rotated(part, cos_t[:, cols], sin_t[:, cols])
            kv_out[column(k, head), cols] = jnp.where(turned, spun, part.astype(F32)).astype(BF16)
    ex_s.recv()
    total = dg_x[0]
    for i in range(1, TX):
        total = total + dg_x[i]
    dg_y[place.ty] = total
    for d in range(1, TY):
        gain_link.go(dg_y.at[place.ty], dg_y.at[place.ty], 0, {"ty": wrap(place.ty + d, TY)})
    proj_grad.finish()
    ex_o.recv()
    gain_link.recv()
    total = dg_y[0]
    for j in range(1, TY):
        total = total + dg_y[j]
    dg_out[0] = total[0:1]
    dg_out[1] = total[1:2]
    for item in (ex_h, ex_d, ex_r, ex_q, ex_o, ex_s, gather, w_gate, w_up, w_down, w_proj,
                 ag_e, ag_n, rs3, gain_link, down_grad, gate_grad, proj_grad):
        item.done()


def store_kernel(resid, dh, q_t, kv_t, dgu, dwd, dproj, dg,
                 resid_o, dh_o, q_o, kv_o, dga_o, dgb_o, dwg_o, dwu_o, dwd_o, dwq_o, dwkv_o, sems):
    ffn = dwg_o.shape[1]
    nq, nkv = q_o.shape[0], kv_o.shape[0]
    moves = [(dgu.at[:, pl.ds(0, ffn)], dwg_o), (dgu.at[:, pl.ds(ffn, ffn)], dwu_o), (dwd, dwd_o), (resid, resid_o), (dh, dh_o),
             (q_t, q_o), (kv_t, kv_o), (dproj.at[pl.ds(0, nq)], dwq_o), (dproj.at[pl.ds(nq, nkv)], dwkv_o),
             (dg.at[0], dga_o), (dg.at[1], dgb_o)]
    stores = [pltpu.make_async_copy(src, dst, sems.at[k]) for k, (src, dst) in enumerate(moves)]
    for copy in stores:
        copy.start()
    for copy in stores:
        copy.wait()


HBM_SPEC = pl.BlockSpec(memory_space=pl.ANY)


VMEM_SPEC = pl.BlockSpec(memory_space=pltpu.VMEM)


def call(kernel, number, ins, outs, scratch):
    in_spec, out_spec = (HBM_SPEC, VMEM_SPEC) if number is not None else (VMEM_SPEC, HBM_SPEC)
    shape_of = pltpu.VMEM if number is not None else jax.ShapeDtypeStruct
    return pl.pallas_call(
        kernel, out_shape=[shape_of(shape, dtype) for shape, dtype in outs],
        in_specs=[in_spec] * len(ins), out_specs=[out_spec] * len(outs), scratch_shapes=scratch,
        compiler_params=pltpu.CompilerParams(collective_id=number, has_side_effects=number is not None,
                                             vmem_limit_bytes=(59 if number is not None else 4) * 2 ** 20),
        name=kernel.__name__)(*ins)


def solution(mesh):
    def local_step(hidden, positions, g_ffn, w_gate, w_up, w_down, g_attn, w_q, w_kv, grad_h2, grad_q, grad_kv):
        rows, width = hidden.shape
        model_dim = width * TX
        ffn = w_gate.shape[1]
        head_dim = w_q.shape[2]
        tokens = positions.shape[0]

        def features(value):
            return value.transpose(1, 2, 0).reshape(-1, value.shape[0])

        def unfeatures(value):
            return value.reshape(-1, head_dim, value.shape[1]).transpose(2, 0, 1)

        dq, dkv, wq, wkv = features(grad_q), features(grad_kv), features(w_q), features(w_kv)
        nq = dq.shape[0]
        proj = nq + dkv.shape[0]
        own = rows // TX
        inv_freq = ROPE_BASE ** (-np.arange(0, head_dim, 2) / head_dim)
        freq = np.repeat(inv_freq, 2).astype(np.float32)[:, None]
        own = (own, model_dim)
        whole = (tokens, model_dim)
        piece = (TX, own[0], width)
        tile = tokens // TX
        wide = (TX, proj, tile)
        flat = (rows, width)
        gain = (TX, 2, width)
        vmem = [(whole, BF16), ((model_dim, 2 * ffn), BF16), ((ffn, model_dim), BF16), ((proj, model_dim), BF16),
                ((tokens, 2 * ffn), BF16), ((tokens, ffn), BF16), ((proj, tokens), BF16),
                (whole, BF16), (whole, BF16), (whole, BF16), (wide, BF16), (wide, BF16), ((proj, width), BF16),
                (piece, BF16), (piece, BF16), (piece, BF16), (piece, BF16), (piece, F32), (gain, F32), (gain, F32), (gain, F32),
                ((TY, 2, width), F32), ((head_dim, tokens), F32), ((head_dim, tokens), F32)]
        results = [(piece, BF16), (piece, BF16), ((nq, tokens), BF16), ((proj - nq, tokens), BF16),
                   ((width, 2 * ffn), F32), ((ffn, width), F32), ((proj, width), F32), ((2, 1, width), F32)]
        entering = (hidden.reshape(piece), dq, dkv, positions.reshape(1, tokens), freq, g_ffn, g_attn)
        outs = call(
            main_kernel, 0,
            [grad_h2.reshape(piece), w_gate, w_up, w_down, wq, wkv, *entering],
            results,
            [pltpu.VMEM(value.shape, value.dtype) for value in entering] + [pltpu.VMEM(shape, dtype) for shape, dtype in vmem]
            + scatter_scratch(*own) * 2 + tx_scratch(ffn, width) + tx_scratch(width, 2 * ffn) + tx_scratch(proj, width)
            + [pltpu.SemaphoreType.DMA((n,)) for n in SEMS.values()])
        gains_out = ((1, width), F32)
        resid, dh, q_t, kv_t, dga, dgb, dwg, dwu, dwd, dwq, dwkv = call(
            store_kernel, None,
            [pltpu.with_memory_space_constraint(value, pltpu.VMEM) for value in outs],
            results[:4] + [gains_out] * 2
            + [((width, ffn), F32), ((width, ffn), F32), ((ffn, width), F32), ((nq, width), F32), ((proj - nq, width), F32)],
            [pltpu.SemaphoreType.DMA((TY,))])
        return (resid.reshape(flat), unfeatures(q_t), unfeatures(kv_t), dh.reshape(flat), dga[0], dgb[0],
                dwg, dwu, dwd, unfeatures(dwq), unfeatures(dwkv))

    row_spec = P(("dp", "ty"), "tx")
    head_spec = P(("dp", "tx"), "ty", None)
    in_specs = (row_spec, P(("dp", "tx")), P("tx"), P("tx", "ty"), P("tx", "ty"), P("ty", "tx"), P("tx"), P("tx", "ty", None), P("tx", "ty", None), row_spec, head_spec, head_spec)
    out_specs = (row_spec, head_spec, head_spec, row_spec, P(("dp", "tx")), P(("dp", "tx")), P(("dp", "tx"), "ty"), P(("dp", "tx"), "ty"), P(("dp", "ty"), "tx"), head_spec, head_spec)
    return jax.shard_map(local_step, mesh=mesh, in_specs=in_specs, out_specs=out_specs, check_vma=False)
```

```python
import jax
import jax.numpy as jnp
import numpy as np
from jax import lax
from jax.experimental import pallas as pl
from jax.experimental.pallas import tpu as pltpu
from jax.sharding import PartitionSpec as P

NORM_EPS = 1e-5
ROPE_BASE = 10000.0
RING = 4
TY = 16
TX = 8
NN = (((1,), (0,)), ((), ()))
TN = (((0,), (0,)), ((), ()))
NT = (((1,), (1,)), ((), ()))
BF16 = jnp.bfloat16
F32 = jnp.float32
ORDER = (2, 3, 1, 0)
SPREAD = (0, 3, 1, 2)
BOTH = (0, 1)
DIRECT = {2: BOTH, 3: (3,), 1: (2,), 0: ()}
SIDES = ((0, 1), (1, -1))
MESH = pl.DeviceIdType.MESH


def wrap(value, size=RING):
    return lax.rem(value + 2 * size, size)


def aligned(start, size, unit=16):
    return pl.ds(pl.multiple_of(start, unit), size)


def chunk(index, size):
    return aligned(index * size, size, size)


def dot(a, b, form):
    return lax.dot_general(a, b, form, preferred_element_type=F32)


class Place:
    def __init__(self):
        self.ty = lax.axis_index("ty")
        self.tx = lax.axis_index("tx")
        self.coord = {"z": self.ty // RING, "y": lax.rem(self.ty, RING), "x": self.tx // 2}
        self.core = lax.rem(self.tx, 2)
        self.sibling = {"tx": self.tx + 1 - 2 * self.core}

    def peer(self, axis, delta):
        c = wrap(self.coord[axis] + delta)
        if axis == "x":
            return {"tx": c * 2 + self.core}
        if axis == "z":
            return {"ty": c * RING + self.coord["y"]}
        return {"ty": self.coord["z"] * RING + c}

    def slot(self, axis, delta, other_axis, other_delta):
        c = {axis: wrap(self.coord[axis] + delta), other_axis: wrap(self.coord[other_axis] + other_delta)}
        return c["z"] * RING + c["y"]


class Link:
    def __init__(self, sems):
        self.send_sem, self.recv_sems = sems

    def make(self, src, dst, index, device):
        return pltpu.make_async_remote_copy(src_ref=src, dst_ref=dst, send_sem=self.send_sem, recv_sem=self.recv_sems.at[index],
                                            device_id=device, device_id_type=MESH)

    def go(self, src, dst, index, device):
        self.make(src, dst, index, device).start()

    def wait(self, ref, index, device):
        self.make(ref, ref, index, device).wait_recv()

    def done(self):
        ref = self.sent()
        self.make(ref, ref, 0, self.place.peer("x", 1)).wait_send()


def enter(devices):
    barrier = pltpu.get_barrier_semaphore()
    for device in devices:
        pl.semaphore_signal(barrier, inc=1, device_id=device, device_id_type=MESH)
    pl.semaphore_wait(barrier, len(devices))


def tx_devices(place):
    return [{"tx": wrap(place.tx + d, TX)} for d in range(1, TX)]


class Exchange(Link):
    def __init__(self, place, piece, out, sems):
        super().__init__(sems)
        self.place, self.piece, self.out = place, piece, out

    def target(self, i):
        return self.out.at[i]

    def send(self):
        place = self.place
        for dx in ORDER:
            for flip in BOTH:
                if dx or flip:
                    to = wrap(place.coord["x"] + dx) * 2 + (1 - place.core if flip else place.core)
                    self.go(self.piece(to), self.target(place.tx), 0, {"tx": to})

    def sent(self):
        return self.out.at[pl.ds(0, self.out.shape[0] - 1)]

    def own(self):
        self.target(self.place.tx)[...] = self.piece(self.place.tx)[...]

    def recv(self):
        self.wait(self.sent(), 0, self.place.sibling)


class TyGather(Link):
    def __init__(self, place, buf, sems):
        super().__init__(sems)
        self.place, self.buf = place, buf
        self.rows = buf.shape[0] // TY

    def message(self, half, phase, d, kind, receiving):
        place = self.place
        first, second = ("z", "y") if half == 0 else ("y", "z")
        axis = second if phase else first
        side = 1 - 2 * (kind % 2)
        hops = (0, 0, -1, 1, 0, 0)[kind]
        if receiving:
            hops = hops - side
        slot = place.slot(first, d, second, hops) if phase else place.slot(first, hops, second, 0)
        q = self.rows // 4
        start = slot * self.rows + 2 * q * half
        if not phase or kind > 1:
            start = start + q * (kind % 2 if kind < 4 else 5 - kind)
        ref = self.buf.at[aligned(start, 2 * q if phase and kind < 2 else q)]
        number = kind + (0 if not phase else 6 + 2 * d if kind < 2 else 12)
        return ref, half * TY + number, place.peer(axis, side)

    def send(self, half, phase, d, kinds=BOTH):
        for kind in kinds:
            ref, index, device = self.message(half, phase, d, kind, False)
            self.go(ref, ref, index, device)

    def recv(self, half, phase, d, kind):
        self.wait(*self.message(half, phase, d, kind, True))

    def sent(self):
        return self.buf.at[pl.ds(0, (TY - 1) * self.rows)]

    def start(self):
        for half in BOTH:
            self.send(half, 0, 0, (0, 1, 5, 4))
        for half in BOTH:
            self.send(half, 1, 0)

    def relay(self, half, phase, d):
        for kind in BOTH:
            self.recv(half, phase, d, kind)
            self.send(half, phase, d, (2 + kind,))

    def opposite(self, half, phase, d):
        for kind in BOTH:
            self.recv(half, phase, d, 2 + kind)

    def step_first(self):
        for half in BOTH:
            self.relay(half, 0, 0)
        for half in BOTH:
            self.recv(half, 0, 0, 4)
            self.send(half, 1, 3)
            self.recv(half, 0, 0, 5)
            self.send(half, 1, 1)

    def step_second(self):
        for half in BOTH:
            self.opposite(half, 0, 0)
            self.send(half, 1, 2)

    def step_forward(self, d):
        for half in BOTH:
            self.relay(half, 1, d)

    def finish(self):
        for half in BOTH:
            for kind in (2, 3):
                _, index, device = self.message(half, 1, 0, kind, True)
                self.wait(self.buf.at[pl.ds(0, self.rows)], index, device)


class TyScatter(Link):
    def __init__(self, place, x, got, made, mid, out, sems):
        super().__init__(sems)
        self.place, self.x, self.got, self.made, self.mid, self.out = place, x, got, made, mid, out
        self.rows = out.shape[0]
        self.q = self.rows // 4

    def axes(self, half, phase):
        return ("z", "y") if half != phase else ("y", "z")

    def part(self, half, phase, d, c, quarter):
        big, small = self.axes(half, 0)
        if phase:
            return self.mid.at[half, c, pl.ds(self.q * quarter, self.q)]
        start = self.place.slot(big, c, small, d) * self.rows + self.q * (2 * half + quarter)
        return self.x.at[aligned(start, self.q)]

    def number(self, half, phase, d):
        return half * 5 + (4 if phase else d)

    def send(self, half, phase, d, kinds=BOTH):
        n = self.number(half, phase, d)
        for kind in kinds:
            if kind < 4:
                c, quarter = ((2, 0), (2, 1), (1, 1), (3, 0))[kind]
                src = self.part(half, phase, d, c, quarter)
            else:
                src = self.made.at[n * 2 + kind - 4]
            self.go(src, self.got.at[n * 6 + kind], self.semaphore(half, phase, d, kind), self.place.peer(self.axes(half, phase)[0], 1 - 2 * (kind % 2)))

    def semaphore(self, half, phase, d, kind):
        if phase:
            return half * 24 + 18 + kind
        return half * 24 + (14 + kind if kind in (2, 3) else 4 * d + kind % 4 + kind // 4 * 2)

    def recv(self, half, phase, d, kind):
        ref = self.got.at[self.number(half, phase, d) * 6 + kind]
        if phase or kind not in (2, 3):
            self.wait(ref, self.semaphore(half, phase, d, kind), self.place.sibling)
        return ref[...].astype(F32)

    def directs(self):
        for half in BOTH:
            for kind in (2, 3):
                self.wait(self.x.at[pl.ds(0, self.rows)], self.semaphore(half, 0, 0, kind), self.place.sibling)

    def relay(self, half, phase, d):
        n = self.number(half, phase, d)
        for kind in BOTH:
            theirs = self.part(half, phase, d, 1 + 2 * kind, kind)[...].astype(F32)
            self.made[n * 2 + kind] = (self.recv(half, phase, d, kind) + theirs).astype(BF16)
            self.send(half, phase, d, (4 + kind,))

    def total(self, half, phase, d, quarter):
        value = self.part(half, phase, d, 0, quarter)[...].astype(F32)
        value = value + self.recv(half, phase, d, 3 - quarter)
        return value + self.recv(half, phase, d, 4 + quarter)

    def sent(self):
        return self.x.at[pl.ds(0, (TY - 1) * self.rows)]

    def start(self):
        for kinds in (BOTH, (2, 3)):
            for d in ORDER:
                for half in BOTH:
                    self.send(half, 0, d, kinds)

    def fill(self, compute):
        for d in ORDER:
            compute(wrap(self.place.coord["z"] + d))
            self.send(0, 0, d, range(4))
            for piece in ORDER:
                self.send(1, 0, piece, DIRECT[d])

    def relays(self, *ds):
        for d in ds:
            for half in BOTH:
                self.relay(half, 0, d)

    def middle(self, *ds):
        if ds[0] == ORDER[0]:
            self.directs()
        for d in ds:
            for half in BOTH:
                for quarter in BOTH:
                    value = self.total(half, 0, d, quarter)
                    self.mid[half, d, pl.ds(self.q * quarter, self.q)] = value.astype(BF16)
                self.send(half, 1, 0, DIRECT[d])

    def last_relay(self):
        for half in BOTH:
            self.relay(half, 1, 0)

    def finish(self):
        for half in BOTH:
            for quarter in BOTH:
                self.out[pl.ds(self.q * (2 * half + quarter), self.q)] = self.total(half, 1, 0, quarter)


SCATTER_SEMS = 60


def scatter_scratch(rows, width):
    q = rows // 4
    return [pltpu.VMEM((SCATTER_SEMS, q, width), BF16), pltpu.VMEM((20, q, width), BF16),
            pltpu.VMEM((2, 4, 2 * q, width), BF16), pltpu.VMEM((rows, width), F32)]


SEMS = dict(h=1, r=1, g=1, s=1, e=1, q=1, d=1, o=1, ty=1, gate=10, up=5, down=10, proj=10, ag1=32, rs1=48, rs2=48, pair=RING,
            local=13, send=22)


class TxGather(Link):
    def __init__(self, place, own, view, sems):
        super().__init__(sems)
        self.place, self.own_ref, (self.view, self.blocks) = place, own, view
        self.rows = own.shape[0]

    def ref(self, delta, part=None):
        owner = wrap(self.place.coord["x"] + delta) * 2 + self.place.core
        half = self.rows // 2
        return self.view(owner, 0, self.rows) if part is None else self.view(owner, part * half, half)

    def sent(self):
        return self.blocks(TX - 1)

    def start(self):
        for kind, side in SIDES:
            self.go(self.own_ref, self.ref(0), kind, self.place.peer("x", side))
        self.go(self.own_ref, self.ref(0), 4, self.place.sibling)

    def share(self, delta):
        self.go(self.ref(delta), self.ref(delta), 4, self.place.sibling)

    def forward(self):
        for kind, side in SIDES:
            self.wait(self.ref(-side), kind, self.place.peer("x", side))
            part = self.ref(-side, kind)
            self.go(part, part, 2 + kind, self.place.peer("x", side))
            self.share(-side)

    def last(self):
        for kind, side in SIDES:
            self.wait(self.ref(2, kind), 2 + kind, self.place.peer("x", side))
        self.share(2)

    def finish(self):
        self.wait(self.blocks(RING), 4, self.place.sibling)


def row_view(ref, block, columns):
    return (lambda owner, start, rows: ref.at[aligned(owner * block + start, rows), columns],
            lambda n: ref.at[pl.ds(0, n * block), columns])


def column_view(ref, width):
    return (lambda owner, start, rows: ref.at[pl.ds(start, rows), chunk(owner, width)],
            lambda n: ref.at[:, pl.ds(0, n * width)])


class Local:
    def __init__(self, sem):
        self.sem = sem
        self.copies = []

    def go(self, src, dst):
        copy = pltpu.make_async_copy(src, dst, self.sem.at[len(self.copies)])
        copy.start()
        self.copies.append(copy)
        return copy


def swap_rows(value):
    size = value.shape[0]
    row = lax.broadcasted_iota(jnp.int32, (size, size), 0)
    col = lax.broadcasted_iota(jnp.int32, (size, size), 1)
    swap = jnp.where(row == col + 1 - 2 * lax.rem(col, 2), 1.0, 0.0).astype(BF16)
    return dot(swap, value, NN)


def rotated(value, cos_t, sin_t):
    return value.astype(F32) * cos_t + swap_rows(value) * sin_t


def join_halves(left, right, swap_left):
    half = left.shape[1] // 2
    lane = lax.broadcasted_iota(jnp.int32, left.shape, 1)
    if swap_left:
        left = pltpu.roll(left, half, 1)
    else:
        right = pltpu.roll(right, half, 1)
    return jnp.where(lane < half, left, right)


def column(i, width):
    return slice(i * width, (i + 1) * width)


class TxScatter(Link):
    def __init__(self, place, piece, give, paired, got, made, out, sems, pair_sems):
        super().__init__(sems)
        self.pair_sems = pair_sems
        self.place, self.piece, self.give, self.paired, self.summed = place, piece, give, paired, give
        self.got, self.made, self.out = got, made, out
        self.half = out.shape[0] // 2

    def owner(self, d, core):
        return wrap(self.place.coord["x"] + d) * 2 + core

    def handover(self, d):
        return pltpu.make_async_remote_copy(
            src_ref=self.give.at[d], dst_ref=self.paired.at[d], send_sem=self.pair_sems.at[d],
            recv_sem=self.recv_sems.at[6 + d], device_id=self.place.sibling, device_id_type=MESH)

    def sent(self):
        return self.got

    def start(self):
        def body(t, carry):
            d = wrap(t + 2)
            self.give[d] = self.piece(self.owner(d, 1 - self.place.core)).astype(BF16)
            self.handover(d).start()
            return carry

        lax.fori_loop(0, RING, body, 0)

    def pair(self):
        def body(t, carry):
            d = wrap(t + 2)
            value = self.piece(self.owner(d, self.place.core))
            self.handover(d).wait()
            self.summed[d] = (value + self.paired[d].astype(F32)).astype(BF16)
            return carry

        lax.fori_loop(0, RING, body, 0)
        self.ring(range(4))

    def ring(self, kinds):
        for kind in kinds:
            if kind < 4:
                d, part = ((2, 0), (2, 1), (1, 1), (3, 0))[kind]
                src = self.summed.at[d, pl.ds(part * self.half, self.half)]
            else:
                src = self.made.at[kind - 4]
            self.go(src, self.got.at[kind], kind, self.place.peer("x", 1 - 2 * (kind % 2)))

    def each(self, step, count, body):
        def run(k, carry):
            body(k * step)
            return carry

        lax.fori_loop(0, count // step, run, 0)

    def relay(self):
        for kind in BOTH:
            self.wait(self.got.at[kind], kind, self.place.peer("x", 1))

            def body(start, kind=kind):
                rows = aligned(start, 32, 32)
                theirs = self.summed[1 + 2 * kind, aligned(kind * self.half + start, 32, 32)]
                self.made[kind, rows] = (self.got[kind, rows].astype(F32) + theirs.astype(F32)).astype(BF16)

            self.each(32, self.half, body)
            self.ring((4 + kind,))

    def finish(self):
        for part in BOTH:
            for kind in (3 - part, 4 + part):
                self.wait(self.got.at[kind], kind, self.place.peer("x", 1))

            def body(start, part=part):
                rows = aligned(start, 32, 32)
                full = aligned(part * self.half + start, 32, 32)
                value = self.summed[0, full].astype(F32) + self.got[3 - part, rows].astype(F32)
                self.out[full] = value + self.got[4 + part, rows].astype(F32)

            self.each(32, self.half, body)


def tx_scratch(rows, width):
    full = pltpu.VMEM((RING, rows, width), BF16)
    return [full, full, pltpu.VMEM((6, rows // 2, width), BF16), pltpu.VMEM((2, rows // 2, width), BF16)]


def main_kernel(dh2, wg, wu, wd, wq, wkv, *rest):
    inputs, outputs, entered, rest = rest[:7], rest[7:15], rest[15:22], rest[22:]
    h, dq, dkv, positions, freq, g_ffn, g_attn = entered
    resid, dh, q_out, kv_out, dgu, dwd, dproj, dg_out = outputs
    (n_all, wgu, wd_all, wqkv_all, ab, u, eq_t, e_all, x1, x2, eq_send, qkv_r, wqkv, h_t, h2_t, dh2_t, dh_t, dres_t,
     g_all, dg_part, dg_x, dg_y, cos_t, sin_t) = rest[:24]
    rest = rest[24:]
    place = Place()
    rs_scratch1, rs_scratch2 = rest[:4], rest[4:8]
    tx_refs = [rest[8 + 4 * k:12 + 4 * k] for k in range(3)]
    recv, recv_names = rest[20:], list(SEMS)
    local = Local(recv[recv_names.index("local")])
    n2_all, x3, qkv_send, gains = x1, x2, eq_send, dg_y.at[0]
    width = h.shape[2]
    model_dim = TX * width
    ffn = wg.shape[1]
    nq = dq.shape[0]
    head = cos_t.shape[0]
    tile = eq_send.shape[2]
    used = []

    def sems(name):
        used.append(name)
        return recv[recv_names.index("send")].at[len(used) - 1], recv[recv_names.index(name)]

    pair_sems = recv[recv_names.index("pair")]
    ex_h = Exchange(place, lambda i: h.at[i], h_t, sems("h"))
    ex_r = Exchange(place, lambda i: h2_t.at[i], resid, sems("r"))
    ex_g = Exchange(place, lambda i: gains, g_all, sems("g"))
    ex_s = Exchange(place, lambda i: dg_part.at[i], dg_x, sems("s"))
    ex_e = Exchange(place, lambda i: eq_send.at[i], eq_send, sems("e"))
    ex_e.target = lambda i: eq_t.at[:, chunk(i, tile)]
    ex_q = Exchange(place, lambda i: qkv_send.at[i], qkv_r, sems("q"))
    ex_d = Exchange(place, lambda i: dh2.at[i], dh2_t, sems("d"))
    ex_o = Exchange(place, lambda i: dh_t.at[i], dh, sems("o"))
    w_gate = TxGather(place, wg, row_view(wgu, width, pl.ds(0, ffn)), sems("gate"))
    w_up = TxGather(place, wu, row_view(wgu, width, pl.ds(ffn, ffn)), sems("up"))
    w_down = TxGather(place, wd, column_view(wd_all, width), sems("down"))
    w_proj = TxGather(place, wqkv, column_view(wqkv_all, width), sems("proj"))
    down_grad = TxScatter(place, lambda i: dot(u[...], e_all[:, chunk(i, width)], TN), *tx_refs[0], dwd, sems("down"), pair_sems)
    gate_grad = TxScatter(place, lambda i: dot(n_all[:, chunk(i, width)], ab[...], TN), *tx_refs[1], dgu, sems("gate"), pair_sems)
    proj_grad = TxScatter(place, lambda i: dot(eq_t[...], n2_all[:, chunk(i, width)], NN), *tx_refs[2], dproj, sems("proj"),
                          pair_sems)
    gain_link = Exchange(place, None, dg_y, sems("ty"))
    gather = TyGather(place, n_all, sems("ag1"))
    ag_e = TyGather(place, e_all, sems("ag1"))
    ag_n = TyGather(place, n2_all, sems("rs1"))
    rs1 = TyScatter(place, x1, *rs_scratch1, sems("rs1"))
    rs2 = TyScatter(place, x2, *rs_scratch2, sems("rs2"))
    rs3 = TyScatter(place, x3, *rs_scratch2, sems("rs2"))
    entries = [local.go(src, dst) for src, dst in zip(inputs, entered)]
    entries += [local.go(wq, wqkv.at[pl.ds(0, nq)]), local.go(wkv, wqkv.at[pl.ds(nq, wkv.shape[0])])]
    enter(tx_devices(place) + [place.peer(axis, d) for axis in ("z", "y") for d in (1, -1)])
    for copy in entries:
        copy.wait()
    gains[0:1] = g_ffn[...].astype(F32).reshape(1, width)
    gains[1:2] = g_attn[...].astype(F32).reshape(1, width)
    ex_g.send()
    ex_h.send()
    own_copies = [local.go(w.own_ref, w.ref(0)) for w in (w_gate, w_up, w_down)]
    own_copies.append(local.go(dh2.at[place.tx], dh2_t.at[place.tx]))
    angles = freq[...] * positions[...].astype(F32)
    odd_row = lax.rem(lax.broadcasted_iota(jnp.int32, angles.shape, 0), 2) == 1
    cos_t[...] = jnp.cos(angles)
    sine = jnp.sin(angles)
    sin_t[...] = jnp.where(odd_row, sine, -sine)
    turned = place.ty < TY // 2
    for base, ref in ((0, dq), (nq, dkv)):
        for k in range(ref.shape[0] // head):
            rows = slice(k * head, (k + 1) * head)
            out_rows = slice(base + k * head, base + (k + 1) * head)
            value = rotated(ref[rows], cos_t[...], -sin_t[...])
            if base:
                value = jnp.where(turned, value, ref[rows].astype(F32))
            for m in range(TX // 2):
                near, far = value[:, column(m, tile)], value[:, column(m + TX // 2, tile)]
                for odd in BOTH:
                    eq_send[2 * m + odd, out_rows] = join_halves(near, far, odd).astype(BF16)
    ex_e.send()
    w_proj.start()
    w_gate.start()
    ex_e.own()
    w_proj.ref(0)[...] = wqkv[...]
    ex_h.own()
    ex_g.own()
    ex_h.recv()
    ex_g.recv()
    ex_g.done()
    mine = aligned(place.ty * gather.rows, gather.rows)

    def inverse_rms(ref):
        squares = 0.0
        for i in range(TX):
            x = ref[i].astype(F32)
            squares = squares + jnp.sum(x * x, axis=1, keepdims=True)
        return lax.rsqrt(squares / model_dim + NORM_EPS)

    inv1 = inverse_rms(h_t)
    for i in range(TX):
        n_all[mine, column(i, width)] = (h_t[i].astype(F32) * inv1 * g_all[i, 0:1]).astype(BF16)
    gather.start()
    gather.step_first()
    w_proj.forward()
    w_up.start()
    ex_e.recv()
    gather.step_second()
    w_gate.forward()
    w_proj.last()
    gather.step_forward(0)
    w_proj.finish()

    def back_projection(k, carry):
        x2[chunk(k, 256)] = dot(eq_t[:, chunk(k, 256)], wqkv_all[...], TN).astype(BF16)
        return carry

    lax.fori_loop(0, 4, back_projection, 0)
    gather.step_forward(3)
    gather.step_forward(1)
    w_up.forward()
    w_down.start()
    gather.step_forward(2)
    rs2.start()
    w_gate.last()
    gather.finish()
    for copy in own_copies:
        copy.wait()
    w_up.last()
    w_gate.finish()
    w_up.finish()

    def gate_up(k, carry):
        rows = chunk(k, 256)
        both = dot(n_all[rows], wgu[...], NN).astype(BF16)
        ab[rows] = both
        gate = both[:, :ffn].astype(F32)
        u[rows] = (gate * jax.nn.sigmoid(gate) * both[:, ffn:].astype(F32)).astype(BF16)
        return carry

    def down(k):
        x1[chunk(k, 256)] = dot(u[chunk(k, 256)], wd_all[...], NN).astype(BF16)

    lax.fori_loop(0, 2, gate_up, 0)
    w_down.forward()
    ex_d.send()
    rs2.relays(*ORDER)
    lax.fori_loop(2, 4, gate_up, 0)
    w_down.last()
    w_down.finish()
    rs1.fill(down)
    rs2.middle(*ORDER)
    rs1.relays(*ORDER)
    rs2.last_relay()
    rs1.middle(2, 3, 1)
    rs2.finish()
    ex_d.recv()
    rs1.middle(0)
    rs1.last_relay()
    rs2.done()
    rs1.finish()
    for i in range(TX):
        h2_t[i] = (h_t[i].astype(F32) + rs1.out[:, column(i, width)]).astype(BF16)
    inv2 = inverse_rms(h2_t)
    inner = 0.0
    for i in range(TX):
        x = h2_t[i].astype(F32)
        grad = rs2.out[:, column(i, width)]
        dg_part[i, 1:2] = jnp.sum(grad * x * inv2, axis=0, keepdims=True)
        inner = inner + jnp.sum(grad * g_all[i, 1:2] * x, axis=1, keepdims=True)
    cubed = inv2 * inv2 * inv2 * (inner / model_dim)
    for i in range(TX):
        grad = rs2.out[:, column(i, width)] * g_all[i, 1:2]
        value = dh2_t[i].astype(F32) + (inv2 * grad - h2_t[i].astype(F32) * cubed)
        dres_t[i] = value
        e_all[mine, column(i, width)] = value.astype(BF16)
    rs1.done()
    ag_e.start()
    for i in range(TX):
        n2_all[mine, column(i, width)] = (h2_t[i].astype(F32) * inv2 * g_all[i, 1:2]).astype(BF16)
    ex_r.send()
    ex_r.own()
    ag_e.step_first()
    ag_e.step_second()
    for d in SPREAD:
        ag_e.step_forward(d)
    ag_n.start()
    ag_e.finish()

    def grad_act(k, carry):
        rows = chunk(k, 256)
        grad = dot(e_all[rows], wd_all[...], NT)
        gate = ab[rows, :ffn].astype(F32)
        up = ab[rows, ffn:].astype(F32)
        sig = jax.nn.sigmoid(gate)
        ab[rows, :ffn] = (grad * up * sig * (1.0 + gate * (1.0 - sig))).astype(BF16)
        ab[rows, ffn:] = (grad * gate * sig).astype(BF16)
        return carry

    def grad_norm(k):
        x3[chunk(k, 256)] = dot(ab[chunk(k, 256)], wgu[...], NT).astype(BF16)

    def project(k, carry):
        value = dot(wqkv_all[...], n2_all[chunk(k, 256)], NT).astype(BF16)
        qkv_send[2 * k] = value[:, :tile]
        qkv_send[2 * k + 1] = value[:, tile:]
        return carry

    ex_r.recv()
    down_grad.start()
    ag_n.step_first()
    down_grad.pair()
    lax.fori_loop(0, 4, grad_act, 0)
    ag_n.step_second()
    gate_grad.start()
    down_grad.relay()
    ag_n.step_forward(0)
    ag_n.step_forward(3)
    ag_n.step_forward(1)
    gate_grad.pair()
    ag_n.step_forward(2)
    rs3.fill(grad_norm)
    down_grad.finish()
    ag_n.finish()
    ex_e.done()
    lax.fori_loop(0, 4, project, 0)
    ex_q.send()
    ex_q.own()
    gate_grad.relay()
    proj_grad.start()
    rs3.relays(*ORDER)
    proj_grad.pair()
    rs3.middle(*ORDER)
    gate_grad.finish()
    rs3.last_relay()
    proj_grad.relay()
    rs3.finish()
    inner = 0.0
    for i in range(TX):
        x = h_t[i].astype(F32)
        grad = rs3.out[:, column(i, width)]
        dg_part[i, 0:1] = jnp.sum(grad * x * inv1, axis=0, keepdims=True)
        inner = inner + jnp.sum(grad * g_all[i, 0:1] * x, axis=1, keepdims=True)
    ex_s.send()
    ex_s.own()
    cubed = inv1 * inv1 * inv1 * (inner / model_dim)
    for i in range(TX):
        grad = rs3.out[:, column(i, width)] * g_all[i, 0:1]
        dh_t[i] = (dres_t[i] + (inv1 * grad - h_t[i].astype(F32) * cubed)).astype(BF16)
    ex_o.send()
    ex_o.own()
    ex_q.recv()
    for m in range(TX):
        even = 2 * (m % RING)
        cols = column(m, tile)
        left, right = qkv_r[even].astype(F32), qkv_r[even + 1].astype(F32)
        value = join_halves(left, right, m >= RING).astype(BF16)
        for k in range(nq // head):
            q_out[column(k, head), cols] = rotated(value[column(k, head)], cos_t[:, cols], sin_t[:, cols]).astype(BF16)
        for k in range(kv_out.shape[0] // head):
            part = value[nq + k * head:nq + (k + 1) * head]
            spun = rotated(part, cos_t[:, cols], sin_t[:, cols])
            kv_out[column(k, head), cols] = jnp.where(turned, spun, part.astype(F32)).astype(BF16)
    ex_s.recv()
    total = dg_x[0]
    for i in range(1, TX):
        total = total + dg_x[i]
    dg_y[place.ty] = total
    for d in range(1, TY):
        gain_link.go(dg_y.at[place.ty], dg_y.at[place.ty], 0, {"ty": wrap(place.ty + d, TY)})
    proj_grad.finish()
    ex_o.recv()
    gain_link.recv()
    total = dg_y[0]
    for j in range(1, TY):
        total = total + dg_y[j]
    dg_out[0] = total[0:1]
    dg_out[1] = total[1:2]
    for item in (ex_h, ex_d, ex_r, ex_q, ex_o, ex_s, gather, w_gate, w_up, w_down, w_proj,
                 ag_e, ag_n, rs3, gain_link, down_grad, gate_grad, proj_grad):
        item.done()


def store_kernel(resid, dh, q_t, kv_t, dgu, dwd, dproj, dg,
                 resid_o, dh_o, q_o, kv_o, dga_o, dgb_o, dwg_o, dwu_o, dwd_o, dwq_o, dwkv_o, sems):
    ffn = dwg_o.shape[1]
    nq, nkv = q_o.shape[0], kv_o.shape[0]
    moves = [(dgu.at[:, pl.ds(0, ffn)], dwg_o), (dgu.at[:, pl.ds(ffn, ffn)], dwu_o), (dwd, dwd_o), (resid, resid_o), (dh, dh_o),
             (q_t, q_o), (kv_t, kv_o), (dproj.at[pl.ds(0, nq)], dwq_o), (dproj.at[pl.ds(nq, nkv)], dwkv_o),
             (dg.at[0], dga_o), (dg.at[1], dgb_o)]
    stores = [pltpu.make_async_copy(src, dst, sems.at[k]) for k, (src, dst) in enumerate(moves)]
    for copy in stores:
        copy.start()
    for copy in stores:
        copy.wait()


HBM_SPEC = pl.BlockSpec(memory_space=pl.ANY)


VMEM_SPEC = pl.BlockSpec(memory_space=pltpu.VMEM)


def call(kernel, number, ins, outs, scratch):
    in_spec, out_spec = (HBM_SPEC, VMEM_SPEC) if number is not None else (VMEM_SPEC, HBM_SPEC)
    shape_of = pltpu.VMEM if number is not None else jax.ShapeDtypeStruct
    return pl.pallas_call(
        kernel, out_shape=[shape_of(shape, dtype) for shape, dtype in outs],
        in_specs=[in_spec] * len(ins), out_specs=[out_spec] * len(outs), scratch_shapes=scratch,
        compiler_params=pltpu.CompilerParams(collective_id=number, has_side_effects=number is not None,
                                             vmem_limit_bytes=(59 if number is not None else 4) * 2 ** 20),
        name=kernel.__name__)(*ins)


def solution(mesh):
    def local_step(hidden, positions, g_ffn, w_gate, w_up, w_down, g_attn, w_q, w_kv, grad_h2, grad_q, grad_kv):
        rows, width = hidden.shape
        model_dim = width * TX
        ffn = w_gate.shape[1]
        head_dim = w_q.shape[2]
        tokens = positions.shape[0]

        def features(value):
            return value.transpose(1, 2, 0).reshape(-1, value.shape[0])

        def unfeatures(value):
            return value.reshape(-1, head_dim, value.shape[1]).transpose(2, 0, 1)

        dq, dkv, wq, wkv = features(grad_q), features(grad_kv), features(w_q), features(w_kv)
        nq = dq.shape[0]
        proj = nq + dkv.shape[0]
        own = rows // TX
        inv_freq = ROPE_BASE ** (-np.arange(0, head_dim, 2) / head_dim)
        freq = np.repeat(inv_freq, 2).astype(np.float32)[:, None]
        own = (own, model_dim)
        whole = (tokens, model_dim)
        piece = (TX, own[0], width)
        tile = tokens // TX
        wide = (TX, proj, tile)
        flat = (rows, width)
        gain = (TX, 2, width)
        vmem = [(whole, BF16), ((model_dim, 2 * ffn), BF16), ((ffn, model_dim), BF16), ((proj, model_dim), BF16),
                ((tokens, 2 * ffn), BF16), ((tokens, ffn), BF16), ((proj, tokens), BF16),
                (whole, BF16), (whole, BF16), (whole, BF16), (wide, BF16), (wide, BF16), ((proj, width), BF16),
                (piece, BF16), (piece, BF16), (piece, BF16), (piece, BF16), (piece, F32), (gain, F32), (gain, F32), (gain, F32),
                ((TY, 2, width), F32), ((head_dim, tokens), F32), ((head_dim, tokens), F32)]
        results = [(piece, BF16), (piece, BF16), ((nq, tokens), BF16), ((proj - nq, tokens), BF16),
                   ((width, 2 * ffn), F32), ((ffn, width), F32), ((proj, width), F32), ((2, 1, width), F32)]
        entering = (hidden.reshape(piece), dq, dkv, positions.reshape(1, tokens), freq, g_ffn, g_attn)
        outs = call(
            main_kernel, 0,
            [grad_h2.reshape(piece), w_gate, w_up, w_down, wq, wkv, *entering],
            results,
            [pltpu.VMEM(value.shape, value.dtype) for value in entering] + [pltpu.VMEM(shape, dtype) for shape, dtype in vmem]
            + scatter_scratch(*own) * 2 + tx_scratch(ffn, width) + tx_scratch(width, 2 * ffn) + tx_scratch(proj, width)
            + [pltpu.SemaphoreType.DMA((n,)) for n in SEMS.values()])
        gains_out = ((1, width), F32)
        resid, dh, q_t, kv_t, dga, dgb, dwg, dwu, dwd, dwq, dwkv = call(
            store_kernel, None,
            [pltpu.with_memory_space_constraint(value, pltpu.VMEM) for value in outs],
            results[:4] + [gains_out] * 2
            + [((width, ffn), F32), ((width, ffn), F32), ((ffn, width), F32), ((nq, width), F32), ((proj - nq, width), F32)],
            [pltpu.SemaphoreType.DMA((TY,))])
        return (resid.reshape(flat), unfeatures(q_t), unfeatures(kv_t), dh.reshape(flat), dga[0], dgb[0],
                dwg, dwu, dwd, unfeatures(dwq), unfeatures(dwkv))

    row_spec = P(("dp", "ty"), "tx")
    head_spec = P(("dp", "tx"), "ty", None)
    in_specs = (row_spec, P(("dp", "tx")), P("tx"), P("tx", "ty"), P("tx", "ty"), P("ty", "tx"), P("tx"), P("tx", "ty", None), P("tx", "ty", None), row_spec, head_spec, head_spec)
    out_specs = (row_spec, head_spec, head_spec, row_spec, P(("dp", "tx")), P(("dp", "tx")), P(("dp", "tx"), "ty"), P(("dp", "tx"), "ty"), P(("dp", "ty"), "tx"), head_spec, head_spec)
    return jax.shard_map(local_step, mesh=mesh, in_specs=in_specs, out_specs=out_specs, check_vma=False)
```

```python
import jax
import jax.numpy as jnp
import numpy as np
from jax import lax
from jax.experimental import pallas as pl
from jax.experimental.pallas import tpu as pltpu
from jax.sharding import PartitionSpec as P

NORM_EPS = 1e-5
ROPE_BASE = 10000.0
RING = 4
TY = 16
TX = 8
NN = (((1,), (0,)), ((), ()))
TN = (((0,), (0,)), ((), ()))
NT = (((1,), (1,)), ((), ()))
BF16 = jnp.bfloat16
F32 = jnp.float32
ORDER = (2, 3, 1, 0)
SPREAD = (0, 3, 1, 2)
BOTH = (0, 1)
LATE = (2, 3)
ROWS = 256
DIRECT = {2: BOTH, 3: (3,), 1: (2,), 0: ()}
SIDES = ((0, 1), (1, -1))
MESH = pl.DeviceIdType.MESH


def wrap(value, size=RING):
    return lax.rem(value + 2 * size, size)


def aligned(start, size, unit=16):
    return pl.ds(pl.multiple_of(start, unit), size)


def chunk(index, size):
    return aligned(index * size, size, size)


def dot(a, b, form):
    return lax.dot_general(a, b, form, preferred_element_type=F32)


class Place:
    def __init__(self):
        self.ty = lax.axis_index("ty")
        self.tx = lax.axis_index("tx")
        self.coord = {"z": self.ty // RING, "y": lax.rem(self.ty, RING), "x": self.tx // 2}
        self.core = lax.rem(self.tx, 2)
        self.sibling = {"tx": self.tx + 1 - 2 * self.core}

    def peer(self, axis, delta):
        c = wrap(self.coord[axis] + delta)
        if axis == "x":
            return {"tx": c * 2 + self.core}
        if axis == "z":
            return {"ty": c * RING + self.coord["y"]}
        return {"ty": self.coord["z"] * RING + c}

    def slot(self, axis, delta, other_axis, other_delta):
        c = {axis: wrap(self.coord[axis] + delta), other_axis: wrap(self.coord[other_axis] + other_delta)}
        return c["z"] * RING + c["y"]


class Link:
    def __init__(self, sems):
        self.send_sem, self.recv_sems = sems

    def make(self, src, dst, index, device):
        return pltpu.make_async_remote_copy(src_ref=src, dst_ref=dst, send_sem=self.send_sem, recv_sem=self.recv_sems.at[index],
                                            device_id=device, device_id_type=MESH)

    def go(self, src, dst, index, device):
        self.make(src, dst, index, device).start()

    def wait(self, ref, index, device):
        self.make(ref, ref, index, device).wait_recv()

    def done(self):
        ref = self.sent()
        self.make(ref, ref, 0, self.place.peer("x", 1)).wait_send()


def enter(devices):
    barrier = pltpu.get_barrier_semaphore()
    for device in devices:
        pl.semaphore_signal(barrier, inc=1, device_id=device, device_id_type=MESH)
    pl.semaphore_wait(barrier, len(devices))


def tx_devices(place):
    return [{"tx": wrap(place.tx + d, TX)} for d in range(1, TX)]


class Exchange(Link):
    def __init__(self, place, piece, out, sems):
        super().__init__(sems)
        self.place, self.piece, self.out = place, piece, out

    def target(self, i):
        return self.out.at[i]

    def send(self):
        place = self.place
        for dx in ORDER:
            for flip in BOTH:
                if dx or flip:
                    to = wrap(place.coord["x"] + dx) * 2 + (1 - place.core if flip else place.core)
                    self.go(self.piece(to), self.target(place.tx), 0, {"tx": to})

    def sent(self):
        return self.out.at[pl.ds(0, self.out.shape[0] - 1)]

    def own(self):
        self.target(self.place.tx)[...] = self.piece(self.place.tx)[...]

    def recv(self):
        self.wait(self.sent(), 0, self.place.sibling)


class TyGather(Link):
    def __init__(self, place, buf, sems):
        super().__init__(sems)
        self.place, self.buf = place, buf
        self.rows = buf.shape[0] // TY

    def message(self, half, phase, d, kind, receiving):
        place = self.place
        first, second = ("z", "y") if half == 0 else ("y", "z")
        axis = second if phase else first
        side = 1 - 2 * (kind % 2)
        hops = (0, 0, -1, 1, 0, 0)[kind]
        if receiving:
            hops = hops - side
        slot = place.slot(first, d, second, hops) if phase else place.slot(first, hops, second, 0)
        q = self.rows // 4
        start = slot * self.rows + 2 * q * half
        if not phase or kind > 1:
            start = start + q * (kind % 2 if kind < 4 else 5 - kind)
        ref = self.buf.at[aligned(start, 2 * q if phase and kind < 2 else q)]
        number = kind + (0 if not phase else 6 + 2 * d if kind < 2 else 12)
        return ref, half * TY + number, place.peer(axis, side)

    def send(self, half, phase, d, kinds=BOTH):
        for kind in kinds:
            ref, index, device = self.message(half, phase, d, kind, False)
            self.go(ref, ref, index, device)

    def recv(self, half, phase, d, kind):
        self.wait(*self.message(half, phase, d, kind, True))

    def sent(self):
        return self.buf.at[pl.ds(0, (TY - 1) * self.rows)]

    def start(self):
        for half in BOTH:
            self.send(half, 0, 0, (0, 1, 5, 4))
        for half in BOTH:
            self.send(half, 1, 0)

    def relay(self, half, phase, d):
        for kind in BOTH:
            self.recv(half, phase, d, kind)
            self.send(half, phase, d, (2 + kind,))

    def opposite(self, half, phase, d):
        for kind in BOTH:
            self.recv(half, phase, d, 2 + kind)

    def step_first(self):
        for half in BOTH:
            self.relay(half, 0, 0)
        for half in BOTH:
            self.recv(half, 0, 0, 4)
            self.send(half, 1, 3)
            self.recv(half, 0, 0, 5)
            self.send(half, 1, 1)

    def step_second(self):
        for half in BOTH:
            self.opposite(half, 0, 0)
            self.send(half, 1, 2)

    def step_forward(self, d):
        for half in BOTH:
            self.relay(half, 1, d)

    def finish(self):
        for half in BOTH:
            for kind in LATE:
                _, index, device = self.message(half, 1, 0, kind, True)
                self.wait(self.buf.at[pl.ds(0, self.rows)], index, device)


class TyScatter(Link):
    def __init__(self, place, x, got, made, mid, out, sems):
        super().__init__(sems)
        self.place, self.x, self.got, self.made, self.mid, self.out = place, x, got, made, mid, out
        self.rows = out.shape[0]
        self.q = self.rows // 4

    def axes(self, half, phase):
        return ("z", "y") if half != phase else ("y", "z")

    def part(self, half, phase, d, c, quarter):
        big, small = self.axes(half, 0)
        if phase:
            return self.mid.at[half, c, pl.ds(self.q * quarter, self.q)]
        start = self.place.slot(big, c, small, d) * self.rows + self.q * (2 * half + quarter)
        return self.x.at[aligned(start, self.q)]

    def number(self, half, phase, d):
        return half * 5 + (4 if phase else d)

    def send(self, half, phase, d, kinds=BOTH):
        n = self.number(half, phase, d)
        for kind in kinds:
            if kind < 4:
                c, quarter = ((2, 0), (2, 1), (1, 1), (3, 0))[kind]
                src = self.part(half, phase, d, c, quarter)
            else:
                src = self.made.at[n * 2 + kind - 4]
            self.go(src, self.got.at[n * 6 + kind], self.semaphore(half, phase, d, kind), self.place.peer(self.axes(half, phase)[0], 1 - 2 * (kind % 2)))

    def semaphore(self, half, phase, d, kind):
        if phase:
            return half * 26 + 20 + kind
        if kind in LATE:
            return half * 26 + TY + kind - (2 if d == ORDER[0] else 0)
        return half * 26 + 4 * d + kind % 4 + kind // 4 * 2

    def recv(self, half, phase, d, kind):
        ref = self.got.at[self.number(half, phase, d) * 6 + kind]
        if phase or kind not in LATE:
            self.wait(ref, self.semaphore(half, phase, d, kind), self.place.sibling)
        return ref[...].astype(F32)

    def directs(self, d, count):
        for half in BOTH:
            for kind in LATE:
                self.wait(self.x.at[pl.ds(0, count * self.q)], self.semaphore(half, 0, d, kind), self.place.sibling)

    def relay(self, half, phase, d):
        n = self.number(half, phase, d)
        for kind in BOTH:
            theirs = self.part(half, phase, d, 1 + 2 * kind, kind)[...].astype(F32)
            self.made[n * 2 + kind] = (self.recv(half, phase, d, kind) + theirs).astype(BF16)
            self.send(half, phase, d, (4 + kind,))

    def total(self, half, phase, d, quarter):
        value = self.part(half, phase, d, 0, quarter)[...].astype(F32)
        value = value + self.recv(half, phase, d, 3 - quarter)
        return value + self.recv(half, phase, d, 4 + quarter)

    def sent(self):
        return self.x.at[pl.ds(0, (TY - 1) * self.rows)]

    def start(self):
        for kinds in (BOTH, LATE):
            for d in ORDER:
                for half in BOTH:
                    self.send(half, 0, d, kinds)

    def fill(self, compute, pieces=ORDER):
        for d in ORDER:
            compute(wrap(self.place.coord["z"] + d))
            self.send(0, 0, d, range(4) if d in pieces else BOTH)
            for piece in ORDER:
                self.send(1, 0, piece, DIRECT[d] if d == ORDER[0] or piece in pieces else ())

    def direct(self, d):
        for half in BOTH:
            self.send(half, 0, d, LATE)

    def relays(self, *ds):
        for d in ds:
            for half in BOTH:
                self.relay(half, 0, d)

    def middle(self, *ds):
        for d in ds:
            if d in LATE:
                self.directs(d, 1 if d == ORDER[0] else RING - 1)
            for half in BOTH:
                for quarter in BOTH:
                    value = self.total(half, 0, d, quarter)
                    self.mid[half, d, pl.ds(self.q * quarter, self.q)] = value.astype(BF16)
                self.send(half, 1, 0, DIRECT[d])

    def last_relay(self):
        for half in BOTH:
            self.relay(half, 1, 0)

    def finish(self):
        for half in BOTH:
            for quarter in BOTH:
                self.out[pl.ds(self.q * (2 * half + quarter), self.q)] = self.total(half, 1, 0, quarter)


SCATTER_SEMS = 60


def scatter_scratch(rows, width):
    q = rows // 4
    return [pltpu.VMEM((SCATTER_SEMS, q, width), BF16), pltpu.VMEM((20, q, width), BF16),
            pltpu.VMEM((2, 4, 2 * q, width), BF16), pltpu.VMEM((rows, width), F32)]


SEMS = dict(h=1, r=1, g=1, s=1, e=1, q=1, d=1, o=1, ty=1, gate=10, up=5, down=10, proj=10, ag1=32, rs1=52, rs2=52, pair=RING,
            local=13, send=22)


class TxGather(Link):
    def __init__(self, place, own, view, sems):
        super().__init__(sems)
        self.place, self.own_ref, (self.view, self.blocks) = place, own, view
        self.rows = own.shape[0]

    def ref(self, delta, part=None):
        owner = wrap(self.place.coord["x"] + delta) * 2 + self.place.core
        half = self.rows // 2
        return self.view(owner, 0, self.rows) if part is None else self.view(owner, part * half, half)

    def sent(self):
        return self.blocks(TX - 1)

    def start(self):
        for kind, side in SIDES:
            self.go(self.own_ref, self.ref(0), kind, self.place.peer("x", side))
        self.go(self.own_ref, self.ref(0), 4, self.place.sibling)

    def share(self, delta):
        self.go(self.ref(delta), self.ref(delta), 4, self.place.sibling)

    def forward(self):
        for kind, side in SIDES:
            self.wait(self.ref(-side), kind, self.place.peer("x", side))
            part = self.ref(-side, kind)
            self.go(part, part, 2 + kind, self.place.peer("x", side))
            self.share(-side)

    def last(self):
        for kind, side in SIDES:
            self.wait(self.ref(2, kind), 2 + kind, self.place.peer("x", side))
        self.share(2)

    def finish(self):
        self.wait(self.blocks(RING), 4, self.place.sibling)


def row_view(ref, block, columns):
    return (lambda owner, start, rows: ref.at[aligned(owner * block + start, rows), columns],
            lambda n: ref.at[pl.ds(0, n * block), columns])


def column_view(ref, width):
    return (lambda owner, start, rows: ref.at[pl.ds(start, rows), chunk(owner, width)],
            lambda n: ref.at[:, pl.ds(0, n * width)])


class Local:
    def __init__(self, sem):
        self.sem = sem
        self.copies = []

    def go(self, src, dst):
        copy = pltpu.make_async_copy(src, dst, self.sem.at[len(self.copies)])
        copy.start()
        self.copies.append(copy)
        return copy


def swap_rows(value):
    size = value.shape[0]
    row = lax.broadcasted_iota(jnp.int32, (size, size), 0)
    col = lax.broadcasted_iota(jnp.int32, (size, size), 1)
    swap = jnp.where(row == col + 1 - 2 * lax.rem(col, 2), 1.0, 0.0).astype(BF16)
    return dot(swap, value, NN)


def rotated(value, cos_t, sin_t):
    return value.astype(F32) * cos_t + swap_rows(value) * sin_t


def join_halves(left, right, swap_left):
    half = left.shape[1] // 2
    lane = lax.broadcasted_iota(jnp.int32, left.shape, 1)
    if swap_left:
        left = pltpu.roll(left, half, 1)
    else:
        right = pltpu.roll(right, half, 1)
    return jnp.where(lane < half, left, right)


def column(i, width):
    return slice(i * width, (i + 1) * width)


class TxScatter(Link):
    def __init__(self, place, piece, give, paired, got, made, out, sems, pair_sems):
        super().__init__(sems)
        self.pair_sems = pair_sems
        self.place, self.piece, self.give, self.paired, self.summed = place, piece, give, paired, give
        self.got, self.made, self.out = got, made, out
        self.half = out.shape[0] // 2

    def owner(self, d, core):
        return wrap(self.place.coord["x"] + d) * 2 + core

    def handover(self, d):
        return pltpu.make_async_remote_copy(
            src_ref=self.give.at[d], dst_ref=self.paired.at[d], send_sem=self.pair_sems.at[d],
            recv_sem=self.recv_sems.at[6 + d], device_id=self.place.sibling, device_id_type=MESH)

    def sent(self):
        return self.got

    def start(self):
        def body(t, carry):
            d = wrap(t + 2)
            self.give[d] = self.piece(self.owner(d, 1 - self.place.core)).astype(BF16)
            self.handover(d).start()
            return carry

        lax.fori_loop(0, RING, body, 0)

    def pair(self):
        def body(t, carry):
            d = wrap(t + 2)
            value = self.piece(self.owner(d, self.place.core))
            self.handover(d).wait()
            self.summed[d] = (value + self.paired[d].astype(F32)).astype(BF16)
            return carry

        lax.fori_loop(0, RING, body, 0)
        self.ring(range(4))

    def ring(self, kinds):
        for kind in kinds:
            if kind < 4:
                d, part = ((2, 0), (2, 1), (1, 1), (3, 0))[kind]
                src = self.summed.at[d, pl.ds(part * self.half, self.half)]
            else:
                src = self.made.at[kind - 4]
            self.go(src, self.got.at[kind], kind, self.place.peer("x", 1 - 2 * (kind % 2)))

    def each(self, step, count, body):
        def run(k, carry):
            body(k * step)
            return carry

        lax.fori_loop(0, count // step, run, 0)

    def relay(self):
        for kind in BOTH:
            self.wait(self.got.at[kind], kind, self.place.peer("x", 1))

            def body(start, kind=kind):
                rows = aligned(start, 32, 32)
                theirs = self.summed[1 + 2 * kind, aligned(kind * self.half + start, 32, 32)]
                self.made[kind, rows] = (self.got[kind, rows].astype(F32) + theirs.astype(F32)).astype(BF16)

            self.each(32, self.half, body)
            self.ring((4 + kind,))

    def finish(self):
        for part in BOTH:
            for kind in (3 - part, 4 + part):
                self.wait(self.got.at[kind], kind, self.place.peer("x", 1))

            def body(start, part=part):
                rows = aligned(start, 32, 32)
                full = aligned(part * self.half + start, 32, 32)
                value = self.summed[0, full].astype(F32) + self.got[3 - part, rows].astype(F32)
                self.out[full] = value + self.got[4 + part, rows].astype(F32)

            self.each(32, self.half, body)


def tx_scratch(rows, width):
    full = pltpu.VMEM((RING, rows, width), BF16)
    return [full, full, pltpu.VMEM((6, rows // 2, width), BF16), pltpu.VMEM((2, rows // 2, width), BF16)]


def main_kernel(dh2, wg, wu, wd, wq, wkv, *rest):
    inputs, outputs, entered, rest = rest[:7], rest[7:15], rest[15:22], rest[22:]
    h, dq, dkv, positions, freq, g_ffn, g_attn = entered
    resid, dh, q_out, kv_out, dgu, dwd, dproj, dg_out = outputs
    (n_all, wgu, wd_all, wqkv_all, ab, u, eq_t, e_all, x1, x2, eq_send, qkv_r, wqkv, h_t, h2_t, dh2_t, dh_t, dres_t,
     g_all, dg_part, dg_x, dg_y, cos_t, sin_t) = rest[:24]
    rest = rest[24:]
    place = Place()
    rs_scratch1, rs_scratch2 = rest[:4], rest[4:8]
    tx_refs = [rest[8 + 4 * k:12 + 4 * k] for k in range(3)]
    recv, recv_names = rest[20:], list(SEMS)
    local = Local(recv[recv_names.index("local")])
    n2_all, x3, qkv_send, gains = x1, x2, eq_send, dg_y.at[0]
    width = h.shape[2]
    model_dim = TX * width
    ffn = wg.shape[1]
    nq = dq.shape[0]
    head = cos_t.shape[0]
    tile = eq_send.shape[2]
    used = []

    def sems(name):
        used.append(name)
        return recv[recv_names.index("send")].at[len(used) - 1], recv[recv_names.index(name)]

    pair_sems = recv[recv_names.index("pair")]
    ex_h = Exchange(place, lambda i: h.at[i], h_t, sems("h"))
    ex_r = Exchange(place, lambda i: h2_t.at[i], resid, sems("r"))
    ex_g = Exchange(place, lambda i: gains, g_all, sems("g"))
    ex_s = Exchange(place, lambda i: dg_part.at[i], dg_x, sems("s"))
    ex_e = Exchange(place, lambda i: eq_send.at[i], eq_send, sems("e"))
    ex_e.target = lambda i: eq_t.at[:, chunk(i, tile)]
    ex_q = Exchange(place, lambda i: qkv_send.at[i], qkv_r, sems("q"))
    ex_d = Exchange(place, lambda i: dh2.at[i], dh2_t, sems("d"))
    ex_o = Exchange(place, lambda i: dh_t.at[i], dh, sems("o"))
    w_gate = TxGather(place, wg, row_view(wgu, width, pl.ds(0, ffn)), sems("gate"))
    w_up = TxGather(place, wu, row_view(wgu, width, pl.ds(ffn, ffn)), sems("up"))
    w_down = TxGather(place, wd, column_view(wd_all, width), sems("down"))
    w_proj = TxGather(place, wqkv, column_view(wqkv_all, width), sems("proj"))
    down_grad = TxScatter(place, lambda i: dot(u[...], e_all[:, chunk(i, width)], TN), *tx_refs[0], dwd, sems("down"), pair_sems)
    gate_grad = TxScatter(place, lambda i: dot(n_all[:, chunk(i, width)], ab[...], TN), *tx_refs[1], dgu, sems("gate"), pair_sems)
    proj_grad = TxScatter(place, lambda i: dot(eq_t[...], n2_all[:, chunk(i, width)], NN), *tx_refs[2], dproj, sems("proj"),
                          pair_sems)
    gain_link = Exchange(place, None, dg_y, sems("ty"))
    gather = TyGather(place, n_all, sems("ag1"))
    ag_e = TyGather(place, e_all, sems("ag1"))
    ag_n = TyGather(place, n2_all, sems("rs1"))
    rs1 = TyScatter(place, x1, *rs_scratch1, sems("rs1"))
    rs2 = TyScatter(place, x2, *rs_scratch2, sems("rs2"))
    rs3 = TyScatter(place, x3, *rs_scratch2, sems("rs2"))
    entries = [local.go(src, dst) for src, dst in zip(inputs, entered)]
    entries += [local.go(wq, wqkv.at[pl.ds(0, nq)]), local.go(wkv, wqkv.at[pl.ds(nq, wkv.shape[0])])]
    enter(tx_devices(place) + [place.peer(axis, d) for axis in ("z", "y") for d in (1, -1)])
    for copy in entries:
        copy.wait()
    gains[0:1] = g_ffn[...].astype(F32).reshape(1, width)
    gains[1:2] = g_attn[...].astype(F32).reshape(1, width)
    ex_g.send()
    ex_h.send()
    own_copies = [local.go(w.own_ref, w.ref(0)) for w in (w_gate, w_up, w_down)]
    own_copies.append(local.go(dh2.at[place.tx], dh2_t.at[place.tx]))
    angles = freq[...] * positions[...].astype(F32)
    odd_row = lax.rem(lax.broadcasted_iota(jnp.int32, angles.shape, 0), 2) == 1
    cos_t[...] = jnp.cos(angles)
    sine = jnp.sin(angles)
    sin_t[...] = jnp.where(odd_row, sine, -sine)
    turned = place.ty < TY // 2
    for base, ref in ((0, dq), (nq, dkv)):
        for k in range(ref.shape[0] // head):
            rows = slice(k * head, (k + 1) * head)
            out_rows = slice(base + k * head, base + (k + 1) * head)
            value = rotated(ref[rows], cos_t[...], -sin_t[...])
            if base:
                value = jnp.where(turned, value, ref[rows].astype(F32))
            for m in range(TX // 2):
                near, far = value[:, column(m, tile)], value[:, column(m + TX // 2, tile)]
                for odd in BOTH:
                    eq_send[2 * m + odd, out_rows] = join_halves(near, far, odd).astype(BF16)
    ex_e.send()
    w_proj.start()
    w_gate.start()
    ex_e.own()
    w_proj.ref(0)[...] = wqkv[...]
    ex_h.own()
    ex_g.own()
    ex_h.recv()
    ex_g.recv()
    ex_g.done()
    mine = aligned(place.ty * gather.rows, gather.rows)

    def inverse_rms(ref):
        squares = 0.0
        for i in range(TX):
            x = ref[i].astype(F32)
            squares = squares + jnp.sum(x * x, axis=1, keepdims=True)
        return lax.rsqrt(squares / model_dim + NORM_EPS)

    inv1 = inverse_rms(h_t)
    for i in range(TX):
        n_all[mine, column(i, width)] = (h_t[i].astype(F32) * inv1 * g_all[i, 0:1]).astype(BF16)
    gather.start()
    gather.step_first()
    w_proj.forward()
    w_up.start()
    ex_e.recv()
    gather.step_second()
    w_gate.forward()
    w_proj.last()
    gather.step_forward(0)
    w_proj.finish()

    def back_projection(k, carry):
        x2[chunk(k, ROWS)] = dot(eq_t[:, chunk(k, ROWS)], wqkv_all[...], TN).astype(BF16)
        return carry

    lax.fori_loop(0, RING, back_projection, 0)
    gather.step_forward(3)
    gather.step_forward(1)
    w_up.forward()
    w_down.start()
    gather.step_forward(2)
    rs2.start()
    w_gate.last()
    gather.finish()
    for copy in own_copies:
        copy.wait()
    w_up.last()
    w_gate.finish()
    w_up.finish()

    def gate_up(k, carry):
        rows = chunk(k, ROWS)
        both = dot(n_all[rows], wgu[...], NN).astype(BF16)
        ab[rows] = both
        gate = both[:, :ffn].astype(F32)
        u[rows] = (gate * jax.nn.sigmoid(gate) * both[:, ffn:].astype(F32)).astype(BF16)
        return carry

    def down(k):
        x1[chunk(k, ROWS)] = dot(u[chunk(k, ROWS)], wd_all[...], NN).astype(BF16)

    lax.fori_loop(0, 2, gate_up, 0)
    w_down.forward()
    ex_d.send()
    rs2.relays(*ORDER)
    lax.fori_loop(2, 4, gate_up, 0)
    w_down.last()
    w_down.finish()
    rs1.fill(down)
    rs2.middle(*ORDER)
    rs1.relays(*ORDER)
    rs2.last_relay()
    rs1.middle(2, 3, 1)
    rs2.finish()
    ex_d.recv()
    rs1.middle(0)
    rs1.last_relay()
    rs2.done()
    rs1.finish()
    for i in range(TX):
        h2_t[i] = (h_t[i].astype(F32) + rs1.out[:, column(i, width)]).astype(BF16)
    inv2 = inverse_rms(h2_t)
    inner = 0.0
    for i in range(TX):
        x = h2_t[i].astype(F32)
        grad = rs2.out[:, column(i, width)]
        dg_part[i, 1:2] = jnp.sum(grad * x * inv2, axis=0, keepdims=True)
        inner = inner + jnp.sum(grad * g_all[i, 1:2] * x, axis=1, keepdims=True)
    cubed = inv2 * inv2 * inv2 * (inner / model_dim)
    for i in range(TX):
        grad = rs2.out[:, column(i, width)] * g_all[i, 1:2]
        value = dh2_t[i].astype(F32) + (inv2 * grad - h2_t[i].astype(F32) * cubed)
        dres_t[i] = value
        e_all[mine, column(i, width)] = value.astype(BF16)
    rs1.done()
    ag_e.start()
    for i in range(TX):
        n2_all[mine, column(i, width)] = (h2_t[i].astype(F32) * inv2 * g_all[i, 1:2]).astype(BF16)
    ex_r.send()
    ex_r.own()
    ag_e.step_first()
    ag_e.step_second()
    for d in SPREAD:
        ag_e.step_forward(d)
    ag_n.start()
    ag_e.finish()

    def grad_act(k, carry):
        rows = chunk(k, ROWS)
        grad = dot(e_all[rows], wd_all[...], NT)
        gate = ab[rows, :ffn].astype(F32)
        up = ab[rows, ffn:].astype(F32)
        sig = jax.nn.sigmoid(gate)
        ab[rows, :ffn] = (grad * up * sig * (1.0 + gate * (1.0 - sig))).astype(BF16)
        ab[rows, ffn:] = (grad * gate * sig).astype(BF16)
        return carry

    def grad_norm(k):
        x3[chunk(k, ROWS)] = dot(ab[chunk(k, ROWS)], wgu[...], NT).astype(BF16)

    def project(k, carry):
        value = dot(wqkv_all[...], n2_all[chunk(k, ROWS)], NT).astype(BF16)
        qkv_send[2 * k] = value[:, :tile]
        qkv_send[2 * k + 1] = value[:, tile:]
        return carry

    ex_r.recv()
    down_grad.start()
    ag_n.step_first()
    down_grad.pair()
    lax.fori_loop(0, RING, grad_act, 0)
    ag_n.step_second()
    gate_grad.start()
    down_grad.relay()
    ag_n.step_forward(0)
    ag_n.step_forward(3)
    ag_n.step_forward(1)
    gate_grad.pair()
    ag_n.step_forward(2)
    rs3.fill(grad_norm, ORDER[:1])
    ag_n.finish()
    ex_e.done()
    lax.fori_loop(0, RING, project, 0)
    rs3.relays(2)
    rs3.direct(3)
    ex_q.send()
    ex_q.own()
    rs3.relays(3)
    rs3.direct(1)
    gate_grad.relay()
    proj_grad.start()
    rs3.middle(2)
    rs3.relays(1)
    rs3.direct(0)
    rs3.relays(0)
    proj_grad.pair()
    down_grad.finish()
    rs3.middle(3, 1)
    rs3.last_relay()
    rs3.middle(0)
    gate_grad.finish()
    proj_grad.relay()
    rs3.finish()
    inner = 0.0
    for i in range(TX):
        x = h_t[i].astype(F32)
        grad = rs3.out[:, column(i, width)]
        dg_part[i, 0:1] = jnp.sum(grad * x * inv1, axis=0, keepdims=True)
        inner = inner + jnp.sum(grad * g_all[i, 0:1] * x, axis=1, keepdims=True)
    ex_s.send()
    ex_s.own()
    cubed = inv1 * inv1 * inv1 * (inner / model_dim)
    for i in range(TX):
        grad = rs3.out[:, column(i, width)] * g_all[i, 0:1]
        dh_t[i] = (dres_t[i] + (inv1 * grad - h_t[i].astype(F32) * cubed)).astype(BF16)
    ex_o.send()
    ex_o.own()
    ex_q.recv()
    for m in range(TX):
        even = 2 * (m % RING)
        cols = column(m, tile)
        left, right = qkv_r[even].astype(F32), qkv_r[even + 1].astype(F32)
        value = join_halves(left, right, m >= RING).astype(BF16)
        for k in range(nq // head):
            q_out[column(k, head), cols] = rotated(value[column(k, head)], cos_t[:, cols], sin_t[:, cols]).astype(BF16)
        for k in range(kv_out.shape[0] // head):
            part = value[nq + k * head:nq + (k + 1) * head]
            spun = rotated(part, cos_t[:, cols], sin_t[:, cols])
            kv_out[column(k, head), cols] = jnp.where(turned, spun, part.astype(F32)).astype(BF16)
    ex_s.recv()
    total = dg_x[0]
    for i in range(1, TX):
        total = total + dg_x[i]
    dg_y[place.ty] = total
    for d in range(1, TY):
        gain_link.go(dg_y.at[place.ty], dg_y.at[place.ty], 0, {"ty": wrap(place.ty + d, TY)})
    proj_grad.finish()
    ex_o.recv()
    gain_link.recv()
    total = dg_y[0]
    for j in range(1, TY):
        total = total + dg_y[j]
    dg_out[0] = total[0:1]
    dg_out[1] = total[1:2]
    for item in (ex_h, ex_d, ex_r, ex_q, ex_o, ex_s, gather, w_gate, w_up, w_down, w_proj,
                 ag_e, ag_n, rs3, gain_link, down_grad, gate_grad, proj_grad):
        item.done()


def store_kernel(resid, dh, q_t, kv_t, dgu, dwd, dproj, dg,
                 resid_o, dh_o, q_o, kv_o, dga_o, dgb_o, dwg_o, dwu_o, dwd_o, dwq_o, dwkv_o, sems):
    ffn = dwg_o.shape[1]
    nq, nkv = q_o.shape[0], kv_o.shape[0]
    moves = [(dgu.at[:, pl.ds(0, ffn)], dwg_o), (dgu.at[:, pl.ds(ffn, ffn)], dwu_o), (dwd, dwd_o), (resid, resid_o), (dh, dh_o),
             (q_t, q_o), (kv_t, kv_o), (dproj.at[pl.ds(0, nq)], dwq_o), (dproj.at[pl.ds(nq, nkv)], dwkv_o),
             (dg.at[0], dga_o), (dg.at[1], dgb_o)]
    stores = [pltpu.make_async_copy(src, dst, sems.at[k]) for k, (src, dst) in enumerate(moves)]
    for copy in stores:
        copy.start()
    for copy in stores:
        copy.wait()


HBM_SPEC = pl.BlockSpec(memory_space=pl.ANY)


VMEM_SPEC = pl.BlockSpec(memory_space=pltpu.VMEM)


def call(kernel, number, ins, outs, scratch):
    in_spec, out_spec = (HBM_SPEC, VMEM_SPEC) if number is not None else (VMEM_SPEC, HBM_SPEC)
    shape_of = pltpu.VMEM if number is not None else jax.ShapeDtypeStruct
    return pl.pallas_call(
        kernel, out_shape=[shape_of(shape, dtype) for shape, dtype in outs],
        in_specs=[in_spec] * len(ins), out_specs=[out_spec] * len(outs), scratch_shapes=scratch,
        compiler_params=pltpu.CompilerParams(collective_id=number, has_side_effects=number is not None,
                                             vmem_limit_bytes=(59 if number is not None else 4) * 2 ** 20),
        name=kernel.__name__)(*ins)


def solution(mesh):
    def local_step(hidden, positions, g_ffn, w_gate, w_up, w_down, g_attn, w_q, w_kv, grad_h2, grad_q, grad_kv):
        rows, width = hidden.shape
        model_dim = width * TX
        ffn = w_gate.shape[1]
        head_dim = w_q.shape[2]
        tokens = positions.shape[0]

        def features(value):
            return value.transpose(1, 2, 0).reshape(-1, value.shape[0])

        def unfeatures(value):
            return value.reshape(-1, head_dim, value.shape[1]).transpose(2, 0, 1)

        dq, dkv, wq, wkv = features(grad_q), features(grad_kv), features(w_q), features(w_kv)
        nq = dq.shape[0]
        proj = nq + dkv.shape[0]
        own = rows // TX
        inv_freq = ROPE_BASE ** (-np.arange(0, head_dim, 2) / head_dim)
        freq = np.repeat(inv_freq, 2).astype(np.float32)[:, None]
        own = (own, model_dim)
        whole = (tokens, model_dim)
        piece = (TX, own[0], width)
        tile = tokens // TX
        wide = (TX, proj, tile)
        flat = (rows, width)
        gain = (TX, 2, width)
        vmem = [(whole, BF16), ((model_dim, 2 * ffn), BF16), ((ffn, model_dim), BF16), ((proj, model_dim), BF16),
                ((tokens, 2 * ffn), BF16), ((tokens, ffn), BF16), ((proj, tokens), BF16),
                (whole, BF16), (whole, BF16), (whole, BF16), (wide, BF16), (wide, BF16), ((proj, width), BF16),
                (piece, BF16), (piece, BF16), (piece, BF16), (piece, BF16), (piece, F32), (gain, F32), (gain, F32), (gain, F32),
                ((TY, 2, width), F32), ((head_dim, tokens), F32), ((head_dim, tokens), F32)]
        results = [(piece, BF16), (piece, BF16), ((nq, tokens), BF16), ((proj - nq, tokens), BF16),
                   ((width, 2 * ffn), F32), ((ffn, width), F32), ((proj, width), F32), ((2, 1, width), F32)]
        entering = (hidden.reshape(piece), dq, dkv, positions.reshape(1, tokens), freq, g_ffn, g_attn)
        outs = call(
            main_kernel, 0,
            [grad_h2.reshape(piece), w_gate, w_up, w_down, wq, wkv, *entering],
            results,
            [pltpu.VMEM(value.shape, value.dtype) for value in entering] + [pltpu.VMEM(shape, dtype) for shape, dtype in vmem]
            + scatter_scratch(*own) * 2 + tx_scratch(ffn, width) + tx_scratch(width, 2 * ffn) + tx_scratch(proj, width)
            + [pltpu.SemaphoreType.DMA((n,)) for n in SEMS.values()])
        gains_out = ((1, width), F32)
        resid, dh, q_t, kv_t, dga, dgb, dwg, dwu, dwd, dwq, dwkv = call(
            store_kernel, None,
            [pltpu.with_memory_space_constraint(value, pltpu.VMEM) for value in outs],
            results[:4] + [gains_out] * 2
            + [((width, ffn), F32), ((width, ffn), F32), ((ffn, width), F32), ((nq, width), F32), ((proj - nq, width), F32)],
            [pltpu.SemaphoreType.DMA((TY,))])
        return (resid.reshape(flat), unfeatures(q_t), unfeatures(kv_t), dh.reshape(flat), dga[0], dgb[0],
                dwg, dwu, dwd, unfeatures(dwq), unfeatures(dwkv))

    row_spec = P(("dp", "ty"), "tx")
    head_spec = P(("dp", "tx"), "ty", None)
    in_specs = (row_spec, P(("dp", "tx")), P("tx"), P("tx", "ty"), P("tx", "ty"), P("ty", "tx"), P("tx"), P("tx", "ty", None), P("tx", "ty", None), row_spec, head_spec, head_spec)
    out_specs = (row_spec, head_spec, head_spec, row_spec, P(("dp", "tx")), P(("dp", "tx")), P(("dp", "tx"), "ty"), P(("dp", "tx"), "ty"), P(("dp", "ty"), "tx"), head_spec, head_spec)
    return jax.shard_map(local_step, mesh=mesh, in_specs=in_specs, out_specs=out_specs, check_vma=False)
```

```python
import jax
import jax.numpy as jnp
import numpy as np
from jax import lax
from jax.experimental import pallas as pl
from jax.experimental.pallas import tpu as pltpu
from jax.sharding import PartitionSpec as P

NORM_EPS = 1e-5
ROPE_BASE = 10000.0
RING = 4
TY = 16
TX = 8
NN = (((1,), (0,)), ((), ()))
TN = (((0,), (0,)), ((), ()))
NT = (((1,), (1,)), ((), ()))
BF16 = jnp.bfloat16
F32 = jnp.float32
ORDER = (2, 3, 1, 0)
SPREAD = (0, 3, 1, 2)
BOTH = (0, 1)
LATE = (2, 3)
ROWS = 256
DIRECT = {2: BOTH, 3: (3,), 1: (2,), 0: ()}
SIDES = ((0, 1), (1, -1))
MESH = pl.DeviceIdType.MESH


def wrap(value, size=RING):
    return lax.rem(value + 2 * size, size)


def aligned(start, size, unit=16):
    return pl.ds(pl.multiple_of(start, unit), size)


def chunk(index, size):
    return aligned(index * size, size, size)


def dot(a, b, form):
    return lax.dot_general(a, b, form, preferred_element_type=F32)


class Place:
    def __init__(self):
        self.ty = lax.axis_index("ty")
        self.tx = lax.axis_index("tx")
        self.coord = {"z": self.ty // RING, "y": lax.rem(self.ty, RING), "x": self.tx // 2}
        self.core = lax.rem(self.tx, 2)
        self.sibling = {"tx": self.tx + 1 - 2 * self.core}

    def peer(self, axis, delta):
        c = wrap(self.coord[axis] + delta)
        if axis == "x":
            return {"tx": c * 2 + self.core}
        if axis == "z":
            return {"ty": c * RING + self.coord["y"]}
        return {"ty": self.coord["z"] * RING + c}

    def slot(self, axis, delta, other_axis, other_delta):
        c = {axis: wrap(self.coord[axis] + delta), other_axis: wrap(self.coord[other_axis] + other_delta)}
        return c["z"] * RING + c["y"]


class Link:
    def __init__(self, sems):
        self.send_sem, self.recv_sems = sems

    def make(self, src, dst, index, device):
        return pltpu.make_async_remote_copy(src_ref=src, dst_ref=dst, send_sem=self.send_sem, recv_sem=self.recv_sems.at[index],
                                            device_id=device, device_id_type=MESH)

    def go(self, src, dst, index, device):
        self.make(src, dst, index, device).start()

    def wait(self, ref, index, device):
        self.make(ref, ref, index, device).wait_recv()

    def done(self):
        ref = self.sent()
        self.make(ref, ref, 0, self.place.peer("x", 1)).wait_send()


def enter(devices):
    barrier = pltpu.get_barrier_semaphore()
    for device in devices:
        pl.semaphore_signal(barrier, inc=1, device_id=device, device_id_type=MESH)
    pl.semaphore_wait(barrier, len(devices))


def tx_devices(place):
    return [{"tx": wrap(place.tx + d, TX)} for d in range(1, TX)]


class Exchange(Link):
    def __init__(self, place, piece, out, sems):
        super().__init__(sems)
        self.place, self.piece, self.out = place, piece, out

    def target(self, i):
        return self.out.at[i]

    def send(self):
        place = self.place
        for dx in ORDER:
            for flip in BOTH:
                if dx or flip:
                    to = wrap(place.coord["x"] + dx) * 2 + (1 - place.core if flip else place.core)
                    self.go(self.piece(to), self.target(place.tx), 0, {"tx": to})

    def sent(self):
        return self.out.at[pl.ds(0, self.out.shape[0] - 1)]

    def own(self):
        self.target(self.place.tx)[...] = self.piece(self.place.tx)[...]

    def recv(self):
        self.wait(self.sent(), 0, self.place.sibling)


class TyGather(Link):
    def __init__(self, place, buf, sems):
        super().__init__(sems)
        self.place, self.buf = place, buf
        self.rows = buf.shape[0] // TY

    def message(self, half, phase, d, kind, receiving):
        place = self.place
        first, second = ("z", "y") if half == 0 else ("y", "z")
        axis = second if phase else first
        side = 1 - 2 * (kind % 2)
        hops = (0, 0, -1, 1, 0, 0)[kind]
        if receiving:
            hops = hops - side
        slot = place.slot(first, d, second, hops) if phase else place.slot(first, hops, second, 0)
        q = self.rows // 4
        start = slot * self.rows + 2 * q * half
        if not phase or kind > 1:
            start = start + q * (kind % 2 if kind < 4 else 5 - kind)
        ref = self.buf.at[aligned(start, 2 * q if phase and kind < 2 else q)]
        number = kind + (0 if not phase else 6 + 2 * d if kind < 2 else 12)
        return ref, half * TY + number, place.peer(axis, side)

    def send(self, half, phase, d, kinds=BOTH):
        for kind in kinds:
            ref, index, device = self.message(half, phase, d, kind, False)
            self.go(ref, ref, index, device)

    def recv(self, half, phase, d, kind):
        self.wait(*self.message(half, phase, d, kind, True))

    def sent(self):
        return self.buf.at[pl.ds(0, (TY - 1) * self.rows)]

    def start(self):
        for half in BOTH:
            self.send(half, 0, 0, (0, 1, 5, 4))
        for half in BOTH:
            self.send(half, 1, 0)

    def relay(self, half, phase, d):
        for kind in BOTH:
            self.recv(half, phase, d, kind)
            self.send(half, phase, d, (2 + kind,))

    def opposite(self, half, phase, d):
        for kind in BOTH:
            self.recv(half, phase, d, 2 + kind)

    def step_first(self):
        for half in BOTH:
            self.relay(half, 0, 0)
        for half in BOTH:
            self.recv(half, 0, 0, 4)
            self.send(half, 1, 3)
            self.recv(half, 0, 0, 5)
            self.send(half, 1, 1)

    def step_second(self):
        for half in BOTH:
            self.opposite(half, 0, 0)
            self.send(half, 1, 2)

    def step_forward(self, d):
        for half in BOTH:
            self.relay(half, 1, d)

    def finish(self):
        for half in BOTH:
            for kind in LATE:
                _, index, device = self.message(half, 1, 0, kind, True)
                self.wait(self.buf.at[pl.ds(0, self.rows)], index, device)


class TyScatter(Link):
    def __init__(self, place, x, got, made, mid, out, sems):
        super().__init__(sems)
        self.place, self.x, self.got, self.made, self.mid, self.out = place, x, got, made, mid, out
        self.rows = out.shape[0]
        self.q = self.rows // 4

    def axes(self, half, phase):
        return ("z", "y") if half != phase else ("y", "z")

    def part(self, half, phase, d, c, quarter):
        big, small = self.axes(half, 0)
        if phase:
            return self.mid.at[half, c, pl.ds(self.q * quarter, self.q)]
        start = self.place.slot(big, c, small, d) * self.rows + self.q * (2 * half + quarter)
        return self.x.at[aligned(start, self.q)]

    def number(self, half, phase, d):
        return half * 5 + (4 if phase else d)

    def send(self, half, phase, d, kinds=BOTH):
        n = self.number(half, phase, d)
        for kind in kinds:
            if kind < 4:
                c, quarter = ((2, 0), (2, 1), (1, 1), (3, 0))[kind]
                src = self.part(half, phase, d, c, quarter)
            else:
                src = self.made.at[n * 2 + kind - 4]
            self.go(src, self.got.at[n * 6 + kind], self.semaphore(half, phase, d, kind), self.place.peer(self.axes(half, phase)[0], 1 - 2 * (kind % 2)))

    def semaphore(self, half, phase, d, kind):
        return self.number(half, phase, d) * 6 + kind

    def recv(self, half, phase, d, kind):
        ref = self.got.at[self.number(half, phase, d) * 6 + kind]
        self.wait(ref, self.semaphore(half, phase, d, kind), self.place.sibling)
        return ref[...].astype(F32)

    def relay(self, half, phase, d):
        n = self.number(half, phase, d)
        for kind in BOTH:
            theirs = self.part(half, phase, d, 1 + 2 * kind, kind)[...].astype(F32)
            self.made[n * 2 + kind] = (self.recv(half, phase, d, kind) + theirs).astype(BF16)
            self.send(half, phase, d, (4 + kind,))

    def total(self, half, phase, d, quarter):
        value = self.part(half, phase, d, 0, quarter)[...].astype(F32)
        value = value + self.recv(half, phase, d, 3 - quarter)
        return value + self.recv(half, phase, d, 4 + quarter)

    def sent(self):
        return self.x.at[pl.ds(0, (TY - 1) * self.rows)]

    def start(self):
        for kinds in (BOTH, LATE):
            for d in ORDER:
                for half in BOTH:
                    self.send(half, 0, d, kinds)

    def fill(self, compute, pieces=ORDER):
        for d in ORDER:
            compute(wrap(self.place.coord["z"] + d))
            self.send(0, 0, d, range(4) if d in pieces else BOTH)
            for piece in ORDER:
                self.send(1, 0, piece, DIRECT[d] if d == ORDER[0] or piece in pieces else ())

    def direct(self, d):
        for half in BOTH:
            self.send(half, 0, d, LATE)

    def relays(self, *ds):
        for d in ds:
            for half in BOTH:
                self.relay(half, 0, d)

    def middle(self, *ds):
        for d in ds:
            for half in BOTH:
                for quarter in BOTH:
                    value = self.total(half, 0, d, quarter)
                    self.mid[half, d, pl.ds(self.q * quarter, self.q)] = value.astype(BF16)
                self.send(half, 1, 0, DIRECT[d])

    def last_relay(self):
        for half in BOTH:
            self.relay(half, 1, 0)

    def finish(self):
        for half in BOTH:
            for quarter in BOTH:
                self.out[pl.ds(self.q * (2 * half + quarter), self.q)] = self.total(half, 1, 0, quarter)


SCATTER_SEMS = 60


def scatter_scratch(rows, width):
    q = rows // 4
    return [pltpu.VMEM((SCATTER_SEMS, q, width), BF16), pltpu.VMEM((20, q, width), BF16),
            pltpu.VMEM((2, 4, 2 * q, width), BF16), pltpu.VMEM((rows, width), F32)]


SEMS = dict(h=1, r=1, g=1, s=1, e=1, q=1, d=1, o=1, ty=1, gate=10, up=5, down=10, proj=10, ag1=32, rs1=60, rs2=60, pair=RING,
            local=13, send=22)


class TxGather(Link):
    def __init__(self, place, own, view, sems):
        super().__init__(sems)
        self.place, self.own_ref, (self.view, self.blocks) = place, own, view
        self.rows = own.shape[0]

    def ref(self, delta, part=None):
        owner = wrap(self.place.coord["x"] + delta) * 2 + self.place.core
        half = self.rows // 2
        return self.view(owner, 0, self.rows) if part is None else self.view(owner, part * half, half)

    def sent(self):
        return self.blocks(TX - 1)

    def start(self):
        for kind, side in SIDES:
            self.go(self.own_ref, self.ref(0), kind, self.place.peer("x", side))
        self.go(self.own_ref, self.ref(0), 4, self.place.sibling)

    def share(self, delta):
        self.go(self.ref(delta), self.ref(delta), 4, self.place.sibling)

    def forward(self):
        for kind, side in SIDES:
            self.wait(self.ref(-side), kind, self.place.peer("x", side))
            part = self.ref(-side, kind)
            self.go(part, part, 2 + kind, self.place.peer("x", side))
            self.share(-side)

    def last(self):
        for kind, side in SIDES:
            self.wait(self.ref(2, kind), 2 + kind, self.place.peer("x", side))
        self.share(2)

    def finish(self):
        self.wait(self.blocks(RING), 4, self.place.sibling)


def row_view(ref, block, columns):
    return (lambda owner, start, rows: ref.at[aligned(owner * block + start, rows), columns],
            lambda n: ref.at[pl.ds(0, n * block), columns])


def column_view(ref, width):
    return (lambda owner, start, rows: ref.at[pl.ds(start, rows), chunk(owner, width)],
            lambda n: ref.at[:, pl.ds(0, n * width)])


class Local:
    def __init__(self, sem):
        self.sem = sem
        self.copies = []

    def go(self, src, dst):
        copy = pltpu.make_async_copy(src, dst, self.sem.at[len(self.copies)])
        copy.start()
        self.copies.append(copy)
        return copy


def swap_rows(value):
    size = value.shape[0]
    row = lax.broadcasted_iota(jnp.int32, (size, size), 0)
    col = lax.broadcasted_iota(jnp.int32, (size, size), 1)
    swap = jnp.where(row == col + 1 - 2 * lax.rem(col, 2), 1.0, 0.0).astype(BF16)
    return dot(swap, value, NN)


def rotated(value, cos_t, sin_t):
    return value.astype(F32) * cos_t + swap_rows(value) * sin_t


def join_halves(left, right, swap_left):
    half = left.shape[1] // 2
    lane = lax.broadcasted_iota(jnp.int32, left.shape, 1)
    if swap_left:
        left = pltpu.roll(left, half, 1)
    else:
        right = pltpu.roll(right, half, 1)
    return jnp.where(lane < half, left, right)


def column(i, width):
    return slice(i * width, (i + 1) * width)


class TxScatter(Link):
    def __init__(self, place, piece, give, paired, got, made, out, sems, pair_sems):
        super().__init__(sems)
        self.pair_sems = pair_sems
        self.place, self.piece, self.give, self.paired, self.summed = place, piece, give, paired, give
        self.got, self.made, self.out = got, made, out
        self.half = out.shape[0] // 2

    def owner(self, d, core):
        return wrap(self.place.coord["x"] + d) * 2 + core

    def handover(self, d):
        return pltpu.make_async_remote_copy(
            src_ref=self.give.at[d], dst_ref=self.paired.at[d], send_sem=self.pair_sems.at[d],
            recv_sem=self.recv_sems.at[6 + d], device_id=self.place.sibling, device_id_type=MESH)

    def sent(self):
        return self.got

    def start(self):
        def body(t, carry):
            d = wrap(t + 2)
            self.give[d] = self.piece(self.owner(d, 1 - self.place.core)).astype(BF16)
            self.handover(d).start()
            return carry

        lax.fori_loop(0, RING, body, 0)

    def pair(self):
        def body(t, carry):
            d = wrap(t + 2)
            value = self.piece(self.owner(d, self.place.core))
            self.handover(d).wait()
            self.summed[d] = (value + self.paired[d].astype(F32)).astype(BF16)
            return carry

        lax.fori_loop(0, RING, body, 0)
        self.ring(range(4))

    def ring(self, kinds):
        for kind in kinds:
            if kind < 4:
                d, part = ((2, 0), (2, 1), (1, 1), (3, 0))[kind]
                src = self.summed.at[d, pl.ds(part * self.half, self.half)]
            else:
                src = self.made.at[kind - 4]
            self.go(src, self.got.at[kind], kind, self.place.peer("x", 1 - 2 * (kind % 2)))

    def each(self, step, count, body):
        def run(k, carry):
            body(k * step)
            return carry

        lax.fori_loop(0, count // step, run, 0)

    def relay(self):
        for kind in BOTH:
            self.wait(self.got.at[kind], kind, self.place.peer("x", 1))

            def body(start, kind=kind):
                rows = aligned(start, 32, 32)
                theirs = self.summed[1 + 2 * kind, aligned(kind * self.half + start, 32, 32)]
                self.made[kind, rows] = (self.got[kind, rows].astype(F32) + theirs.astype(F32)).astype(BF16)

            self.each(32, self.half, body)
            self.ring((4 + kind,))

    def finish(self):
        for part in BOTH:
            for kind in (3 - part, 4 + part):
                self.wait(self.got.at[kind], kind, self.place.peer("x", 1))

            def body(start, part=part):
                rows = aligned(start, 32, 32)
                full = aligned(part * self.half + start, 32, 32)
                value = self.summed[0, full].astype(F32) + self.got[3 - part, rows].astype(F32)
                self.out[full] = value + self.got[4 + part, rows].astype(F32)

            self.each(32, self.half, body)


def tx_scratch(rows, width):
    full = pltpu.VMEM((RING, rows, width), BF16)
    return [full, full, pltpu.VMEM((6, rows // 2, width), BF16), pltpu.VMEM((2, rows // 2, width), BF16)]


def main_kernel(dh2, wg, wu, wd, wq, wkv, *rest):
    inputs, outputs, entered, rest = rest[:7], rest[7:15], rest[15:22], rest[22:]
    h, dq, dkv, positions, freq, g_ffn, g_attn = entered
    resid, dh, q_out, kv_out, dgu, dwd, dproj, dg_out = outputs
    (n_all, wgu, wd_all, wqkv_all, ab, u, eq_t, e_all, x1, x2, eq_send, qkv_r, wqkv, h_t, h2_t, dh2_t, dh_t, dres_t,
     g_all, dg_part, dg_x, dg_y, cos_t, sin_t) = rest[:24]
    rest = rest[24:]
    place = Place()
    rs_scratch1, rs_scratch2 = rest[:4], rest[4:8]
    tx_refs = [rest[8 + 4 * k:12 + 4 * k] for k in range(3)]
    recv, recv_names = rest[20:], list(SEMS)
    local = Local(recv[recv_names.index("local")])
    n2_all, x3, qkv_send, gains = x1, x2, eq_send, dg_y.at[0]
    width = h.shape[2]
    model_dim = TX * width
    ffn = wg.shape[1]
    nq = dq.shape[0]
    head = cos_t.shape[0]
    tile = eq_send.shape[2]
    used = []

    def sems(name):
        used.append(name)
        return recv[recv_names.index("send")].at[len(used) - 1], recv[recv_names.index(name)]

    pair_sems = recv[recv_names.index("pair")]
    ex_h = Exchange(place, lambda i: h.at[i], h_t, sems("h"))
    ex_r = Exchange(place, lambda i: h2_t.at[i], resid, sems("r"))
    ex_g = Exchange(place, lambda i: gains, g_all, sems("g"))
    ex_s = Exchange(place, lambda i: dg_part.at[i], dg_x, sems("s"))
    ex_e = Exchange(place, lambda i: eq_send.at[i], eq_send, sems("e"))
    ex_e.target = lambda i: eq_t.at[:, chunk(i, tile)]
    ex_q = Exchange(place, lambda i: qkv_send.at[i], qkv_r, sems("q"))
    ex_d = Exchange(place, lambda i: dh2.at[i], dh2_t, sems("d"))
    ex_o = Exchange(place, lambda i: dh_t.at[i], dh, sems("o"))
    w_gate = TxGather(place, wg, row_view(wgu, width, pl.ds(0, ffn)), sems("gate"))
    w_up = TxGather(place, wu, row_view(wgu, width, pl.ds(ffn, ffn)), sems("up"))
    w_down = TxGather(place, wd, column_view(wd_all, width), sems("down"))
    w_proj = TxGather(place, wqkv, column_view(wqkv_all, width), sems("proj"))
    down_grad = TxScatter(place, lambda i: dot(u[...], e_all[:, chunk(i, width)], TN), *tx_refs[0], dwd, sems("down"), pair_sems)
    gate_grad = TxScatter(place, lambda i: dot(n_all[:, chunk(i, width)], ab[...], TN), *tx_refs[1], dgu, sems("gate"), pair_sems)
    proj_grad = TxScatter(place, lambda i: dot(eq_t[...], n2_all[:, chunk(i, width)], NN), *tx_refs[2], dproj, sems("proj"),
                          pair_sems)
    gain_link = Exchange(place, None, dg_y, sems("ty"))
    gather = TyGather(place, n_all, sems("ag1"))
    ag_e = TyGather(place, e_all, sems("ag1"))
    ag_n = TyGather(place, n2_all, sems("rs1"))
    rs1 = TyScatter(place, x1, *rs_scratch1, sems("rs1"))
    rs2 = TyScatter(place, x2, *rs_scratch2, sems("rs2"))
    rs3 = TyScatter(place, x3, *rs_scratch2, sems("rs2"))
    entries = [local.go(src, dst) for src, dst in zip(inputs, entered)]
    entries += [local.go(wq, wqkv.at[pl.ds(0, nq)]), local.go(wkv, wqkv.at[pl.ds(nq, wkv.shape[0])])]
    enter(tx_devices(place) + [place.peer(axis, d) for axis in ("z", "y") for d in (1, -1)])
    for copy in entries:
        copy.wait()
    gains[0:1] = g_ffn[...].astype(F32).reshape(1, width)
    gains[1:2] = g_attn[...].astype(F32).reshape(1, width)
    ex_g.send()
    ex_h.send()
    own_copies = [local.go(w.own_ref, w.ref(0)) for w in (w_gate, w_up, w_down)]
    own_copies.append(local.go(dh2.at[place.tx], dh2_t.at[place.tx]))
    angles = freq[...] * positions[...].astype(F32)
    odd_row = lax.rem(lax.broadcasted_iota(jnp.int32, angles.shape, 0), 2) == 1
    cos_t[...] = jnp.cos(angles)
    sine = jnp.sin(angles)
    sin_t[...] = jnp.where(odd_row, sine, -sine)
    turned = place.ty < TY // 2
    for base, ref in ((0, dq), (nq, dkv)):
        for k in range(ref.shape[0] // head):
            rows = slice(k * head, (k + 1) * head)
            out_rows = slice(base + k * head, base + (k + 1) * head)
            value = rotated(ref[rows], cos_t[...], -sin_t[...])
            if base:
                value = jnp.where(turned, value, ref[rows].astype(F32))
            for m in range(TX // 2):
                near, far = value[:, column(m, tile)], value[:, column(m + TX // 2, tile)]
                for odd in BOTH:
                    eq_send[2 * m + odd, out_rows] = join_halves(near, far, odd).astype(BF16)
    ex_e.send()
    w_proj.start()
    w_gate.start()
    ex_e.own()
    w_proj.ref(0)[...] = wqkv[...]
    ex_h.own()
    ex_g.own()
    ex_h.recv()
    ex_g.recv()
    ex_g.done()
    mine = aligned(place.ty * gather.rows, gather.rows)

    def inverse_rms(ref):
        squares = 0.0
        for i in range(TX):
            x = ref[i].astype(F32)
            squares = squares + jnp.sum(x * x, axis=1, keepdims=True)
        return lax.rsqrt(squares / model_dim + NORM_EPS)

    inv1 = inverse_rms(h_t)
    for i in range(TX):
        n_all[mine, column(i, width)] = (h_t[i].astype(F32) * inv1 * g_all[i, 0:1]).astype(BF16)
    gather.start()
    gather.step_first()
    w_proj.forward()
    w_up.start()
    ex_e.recv()
    gather.step_second()
    w_gate.forward()
    w_proj.last()
    gather.step_forward(0)
    w_proj.finish()

    def back_projection(k, carry):
        x2[chunk(k, ROWS)] = dot(eq_t[:, chunk(k, ROWS)], wqkv_all[...], TN).astype(BF16)
        return carry

    lax.fori_loop(0, RING, back_projection, 0)
    gather.step_forward(3)
    gather.step_forward(1)
    w_up.forward()
    w_down.start()
    gather.step_forward(2)
    rs2.start()
    w_gate.last()
    gather.finish()
    for copy in own_copies:
        copy.wait()
    w_up.last()
    w_gate.finish()
    w_up.finish()

    def gate_up(k, carry):
        rows = chunk(k, ROWS)
        both = dot(n_all[rows], wgu[...], NN).astype(BF16)
        ab[rows] = both
        gate = both[:, :ffn].astype(F32)
        u[rows] = (gate * jax.nn.sigmoid(gate) * both[:, ffn:].astype(F32)).astype(BF16)
        return carry

    def down(k):
        x1[chunk(k, ROWS)] = dot(u[chunk(k, ROWS)], wd_all[...], NN).astype(BF16)

    lax.fori_loop(0, 2, gate_up, 0)
    w_down.forward()
    ex_d.send()
    rs2.relays(*ORDER)
    lax.fori_loop(2, 4, gate_up, 0)
    w_down.last()
    w_down.finish()
    rs1.fill(down)
    rs2.middle(*ORDER)
    rs1.relays(*ORDER)
    rs2.last_relay()
    rs1.middle(2, 3, 1)
    rs2.finish()
    ex_d.recv()
    rs1.middle(0)
    rs1.last_relay()
    rs2.done()
    rs1.finish()
    for i in range(TX):
        h2_t[i] = (h_t[i].astype(F32) + rs1.out[:, column(i, width)]).astype(BF16)
    inv2 = inverse_rms(h2_t)
    inner = 0.0
    for i in range(TX):
        x = h2_t[i].astype(F32)
        grad = rs2.out[:, column(i, width)]
        dg_part[i, 1:2] = jnp.sum(grad * x * inv2, axis=0, keepdims=True)
        inner = inner + jnp.sum(grad * g_all[i, 1:2] * x, axis=1, keepdims=True)
    cubed = inv2 * inv2 * inv2 * (inner / model_dim)
    for i in range(TX):
        grad = rs2.out[:, column(i, width)] * g_all[i, 1:2]
        value = dh2_t[i].astype(F32) + (inv2 * grad - h2_t[i].astype(F32) * cubed)
        dres_t[i] = value
        e_all[mine, column(i, width)] = value.astype(BF16)
    rs1.done()
    ag_e.start()
    for i in range(TX):
        n2_all[mine, column(i, width)] = (h2_t[i].astype(F32) * inv2 * g_all[i, 1:2]).astype(BF16)
    ex_r.send()
    ex_r.own()
    ag_e.step_first()
    ag_e.step_second()
    for d in SPREAD:
        ag_e.step_forward(d)
    ag_n.start()
    ag_e.finish()

    def grad_act(k, carry):
        rows = chunk(k, ROWS)
        grad = dot(e_all[rows], wd_all[...], NT)
        gate = ab[rows, :ffn].astype(F32)
        up = ab[rows, ffn:].astype(F32)
        sig = jax.nn.sigmoid(gate)
        ab[rows, :ffn] = (grad * up * sig * (1.0 + gate * (1.0 - sig))).astype(BF16)
        ab[rows, ffn:] = (grad * gate * sig).astype(BF16)
        return carry

    def grad_norm(k):
        x3[chunk(k, ROWS)] = dot(ab[chunk(k, ROWS)], wgu[...], NT).astype(BF16)

    def project(k, carry):
        value = dot(wqkv_all[...], n2_all[chunk(k, ROWS)], NT).astype(BF16)
        qkv_send[2 * k] = value[:, :tile]
        qkv_send[2 * k + 1] = value[:, tile:]
        return carry

    ex_r.recv()
    down_grad.start()
    ag_n.step_first()
    down_grad.pair()
    lax.fori_loop(0, RING, grad_act, 0)
    ag_n.step_second()
    gate_grad.start()
    down_grad.relay()
    ag_n.step_forward(0)
    ag_n.step_forward(3)
    ag_n.step_forward(1)
    gate_grad.pair()
    ag_n.step_forward(2)
    rs3.fill(grad_norm, ORDER[:1])
    ag_n.finish()
    ex_e.done()
    lax.fori_loop(0, RING, project, 0)
    rs3.relays(2)
    rs3.direct(3)
    ex_q.send()
    ex_q.own()
    rs3.relays(3)
    rs3.direct(1)
    gate_grad.relay()
    proj_grad.start()
    rs3.middle(2)
    rs3.relays(1)
    rs3.direct(0)
    rs3.relays(0)
    proj_grad.pair()
    down_grad.finish()
    rs3.middle(3, 1)
    rs3.last_relay()
    rs3.middle(0)
    gate_grad.finish()
    proj_grad.relay()
    rs3.finish()
    inner = 0.0
    for i in range(TX):
        x = h_t[i].astype(F32)
        grad = rs3.out[:, column(i, width)]
        dg_part[i, 0:1] = jnp.sum(grad * x * inv1, axis=0, keepdims=True)
        inner = inner + jnp.sum(grad * g_all[i, 0:1] * x, axis=1, keepdims=True)
    ex_s.send()
    ex_s.own()
    cubed = inv1 * inv1 * inv1 * (inner / model_dim)
    for i in range(TX):
        grad = rs3.out[:, column(i, width)] * g_all[i, 0:1]
        dh_t[i] = (dres_t[i] + (inv1 * grad - h_t[i].astype(F32) * cubed)).astype(BF16)
    ex_o.send()
    ex_o.own()
    ex_q.recv()
    for m in range(TX):
        even = 2 * (m % RING)
        cols = column(m, tile)
        left, right = qkv_r[even].astype(F32), qkv_r[even + 1].astype(F32)
        value = join_halves(left, right, m >= RING).astype(BF16)
        for k in range(nq // head):
            q_out[column(k, head), cols] = rotated(value[column(k, head)], cos_t[:, cols], sin_t[:, cols]).astype(BF16)
        for k in range(kv_out.shape[0] // head):
            part = value[nq + k * head:nq + (k + 1) * head]
            spun = rotated(part, cos_t[:, cols], sin_t[:, cols])
            kv_out[column(k, head), cols] = jnp.where(turned, spun, part.astype(F32)).astype(BF16)
    ex_s.recv()
    total = dg_x[0]
    for i in range(1, TX):
        total = total + dg_x[i]
    dg_y[place.ty] = total
    for d in range(1, TY):
        gain_link.go(dg_y.at[place.ty], dg_y.at[place.ty], 0, {"ty": wrap(place.ty + d, TY)})
    proj_grad.finish()
    ex_o.recv()
    gain_link.recv()
    total = dg_y[0]
    for j in range(1, TY):
        total = total + dg_y[j]
    dg_out[0] = total[0:1]
    dg_out[1] = total[1:2]
    for item in (ex_h, ex_d, ex_r, ex_q, ex_o, ex_s, gather, w_gate, w_up, w_down, w_proj,
                 ag_e, ag_n, rs3, gain_link, down_grad, gate_grad, proj_grad):
        item.done()


def store_kernel(resid, dh, q_t, kv_t, dgu, dwd, dproj, dg,
                 resid_o, dh_o, q_o, kv_o, dga_o, dgb_o, dwg_o, dwu_o, dwd_o, dwq_o, dwkv_o, sems):
    ffn = dwg_o.shape[1]
    nq, nkv = q_o.shape[0], kv_o.shape[0]
    moves = [(dgu.at[:, pl.ds(0, ffn)], dwg_o), (dgu.at[:, pl.ds(ffn, ffn)], dwu_o), (dwd, dwd_o), (resid, resid_o), (dh, dh_o),
             (q_t, q_o), (kv_t, kv_o), (dproj.at[pl.ds(0, nq)], dwq_o), (dproj.at[pl.ds(nq, nkv)], dwkv_o),
             (dg.at[0], dga_o), (dg.at[1], dgb_o)]
    stores = [pltpu.make_async_copy(src, dst, sems.at[k]) for k, (src, dst) in enumerate(moves)]
    for copy in stores:
        copy.start()
    for copy in stores:
        copy.wait()


HBM_SPEC = pl.BlockSpec(memory_space=pl.ANY)


VMEM_SPEC = pl.BlockSpec(memory_space=pltpu.VMEM)


def call(kernel, number, ins, outs, scratch):
    in_spec, out_spec = (HBM_SPEC, VMEM_SPEC) if number is not None else (VMEM_SPEC, HBM_SPEC)
    shape_of = pltpu.VMEM if number is not None else jax.ShapeDtypeStruct
    return pl.pallas_call(
        kernel, out_shape=[shape_of(shape, dtype) for shape, dtype in outs],
        in_specs=[in_spec] * len(ins), out_specs=[out_spec] * len(outs), scratch_shapes=scratch,
        compiler_params=pltpu.CompilerParams(collective_id=number, has_side_effects=number is not None,
                                             vmem_limit_bytes=(59 if number is not None else 4) * 2 ** 20),
        name=kernel.__name__)(*ins)


def solution(mesh):
    def local_step(hidden, positions, g_ffn, w_gate, w_up, w_down, g_attn, w_q, w_kv, grad_h2, grad_q, grad_kv):
        rows, width = hidden.shape
        model_dim = width * TX
        ffn = w_gate.shape[1]
        head_dim = w_q.shape[2]
        tokens = positions.shape[0]

        def features(value):
            return value.transpose(1, 2, 0).reshape(-1, value.shape[0])

        def unfeatures(value):
            return value.reshape(-1, head_dim, value.shape[1]).transpose(2, 0, 1)

        dq, dkv, wq, wkv = features(grad_q), features(grad_kv), features(w_q), features(w_kv)
        nq = dq.shape[0]
        proj = nq + dkv.shape[0]
        own = rows // TX
        inv_freq = ROPE_BASE ** (-np.arange(0, head_dim, 2) / head_dim)
        freq = np.repeat(inv_freq, 2).astype(np.float32)[:, None]
        own = (own, model_dim)
        whole = (tokens, model_dim)
        piece = (TX, own[0], width)
        tile = tokens // TX
        wide = (TX, proj, tile)
        flat = (rows, width)
        gain = (TX, 2, width)
        vmem = [(whole, BF16), ((model_dim, 2 * ffn), BF16), ((ffn, model_dim), BF16), ((proj, model_dim), BF16),
                ((tokens, 2 * ffn), BF16), ((tokens, ffn), BF16), ((proj, tokens), BF16),
                (whole, BF16), (whole, BF16), (whole, BF16), (wide, BF16), (wide, BF16), ((proj, width), BF16),
                (piece, BF16), (piece, BF16), (piece, BF16), (piece, BF16), (piece, F32), (gain, F32), (gain, F32), (gain, F32),
                ((TY, 2, width), F32), ((head_dim, tokens), F32), ((head_dim, tokens), F32)]
        results = [(piece, BF16), (piece, BF16), ((nq, tokens), BF16), ((proj - nq, tokens), BF16),
                   ((width, 2 * ffn), F32), ((ffn, width), F32), ((proj, width), F32), ((2, 1, width), F32)]
        entering = (hidden.reshape(piece), dq, dkv, positions.reshape(1, tokens), freq, g_ffn, g_attn)
        outs = call(
            main_kernel, 0,
            [grad_h2.reshape(piece), w_gate, w_up, w_down, wq, wkv, *entering],
            results,
            [pltpu.VMEM(value.shape, value.dtype) for value in entering] + [pltpu.VMEM(shape, dtype) for shape, dtype in vmem]
            + scatter_scratch(*own) * 2 + tx_scratch(ffn, width) + tx_scratch(width, 2 * ffn) + tx_scratch(proj, width)
            + [pltpu.SemaphoreType.DMA((n,)) for n in SEMS.values()])
        gains_out = ((1, width), F32)
        resid, dh, q_t, kv_t, dga, dgb, dwg, dwu, dwd, dwq, dwkv = call(
            store_kernel, None,
            [pltpu.with_memory_space_constraint(value, pltpu.VMEM) for value in outs],
            results[:4] + [gains_out] * 2
            + [((width, ffn), F32), ((width, ffn), F32), ((ffn, width), F32), ((nq, width), F32), ((proj - nq, width), F32)],
            [pltpu.SemaphoreType.DMA((TY,))])
        return (resid.reshape(flat), unfeatures(q_t), unfeatures(kv_t), dh.reshape(flat), dga[0], dgb[0],
                dwg, dwu, dwd, unfeatures(dwq), unfeatures(dwkv))

    row_spec = P(("dp", "ty"), "tx")
    head_spec = P(("dp", "tx"), "ty", None)
    in_specs = (row_spec, P(("dp", "tx")), P("tx"), P("tx", "ty"), P("tx", "ty"), P("ty", "tx"), P("tx"), P("tx", "ty", None), P("tx", "ty", None), row_spec, head_spec, head_spec)
    out_specs = (row_spec, head_spec, head_spec, row_spec, P(("dp", "tx")), P(("dp", "tx")), P(("dp", "tx"), "ty"), P(("dp", "tx"), "ty"), P(("dp", "ty"), "tx"), head_spec, head_spec)
    return jax.shard_map(local_step, mesh=mesh, in_specs=in_specs, out_specs=out_specs, check_vma=False)
```
